32 devices in a mesh: dp: 2 (over x), tp: 16 (over z, y, core).
Axes of the slice: x: 2, y: 2, z: 4, core: 2. Of those that a mesh axis runs over, the one named last changes fastest.
Arguments:
- token_ids: int32 [2, 2048], P('dp'), parts along dimension 0
- emb_table: bfloat16 [49152, 2048], P('tp')
- norm_gain: bfloat16 [2048], replicated
- grad_out: bfloat16 [2, 2048, 2048], P('dp', 'tp'), parts along dimension 0
Outputs:
- output 1: bfloat16 [2, 2048, 2048], P('dp', 'tp'), parts along dimension 0
- output 2: float32 [98304, 2048], P(('dp', 'tp')), parts along dimension 0
- output 3: float32 [4096], P('dp'), parts along dimension 0
There are 2 independent parts. The reference program is written for one: setup_inputs(seed, part) draws one part's arguments, and reference() takes and returns one part's arrays. A program takes and returns all parts, laid end to end along the dimension named above; an argument that names none is the same for every part.
All inputs are finite; a program needn't handle non-finite values.
Results may differ from the reference program's by a relative error of at most 0.0084057.
Values are sent between devices in bfloat16 or wider.
A program may use at most 1 GiB of HBM per device.

```python
import jax
import jax.numpy as jnp
from jax import lax

VOCAB_SIZE = 49152
HIDDEN = 2048
BATCH_ROWS = 1
SEQ_LEN = 2048
RMS_EPS = 1e-5


def setup_inputs(seed: int = 0, part: int = 0) -> dict:
    base_key = jax.random.key(seed)
    key_table, key_gain, key_perm, key_ids, key_grad = jax.random.split(base_key, 5)
    popularity = jax.random.permutation(key_perm, VOCAB_SIZE)
    uniform_draws = jax.random.randint(jax.random.fold_in(key_ids, part), (BATCH_ROWS, SEQ_LEN), 1, 1048577)
    ranks = (67108864 // uniform_draws - 64) % VOCAB_SIZE
    token_ids = jnp.take(popularity, ranks).astype(jnp.int32)
    token_ids = token_ids.at[0, 0].set(0).at[BATCH_ROWS - 1, SEQ_LEN - 1].set(VOCAB_SIZE - 1)
    emb_table = jax.random.normal(key_table, (VOCAB_SIZE, HIDDEN), jnp.float32).astype(jnp.bfloat16)
    norm_gain = (1.0 + 0.5 * jax.random.normal(key_gain, (HIDDEN,), jnp.float32)).astype(jnp.bfloat16)
    grad_out = jax.random.normal(jax.random.fold_in(key_grad, part), (BATCH_ROWS, SEQ_LEN, HIDDEN), jnp.float32).astype(jnp.bfloat16)
    return {'token_ids': token_ids, 'emb_table': emb_table, 'norm_gain': norm_gain, 'grad_out': grad_out}


def reference(token_ids, emb_table, norm_gain, grad_out):
    embedded = jnp.take(emb_table, token_ids, axis=0)
    hidden_f32 = embedded.astype(jnp.float32)
    inv_rms = lax.rsqrt(jnp.mean(hidden_f32 * hidden_f32, axis=-1, keepdims=True) + RMS_EPS)
    x_hat = hidden_f32 * inv_rms
    normed = x_hat.astype(jnp.bfloat16) * norm_gain
    grad_f32 = grad_out.astype(jnp.float32)
    grad_gain = jnp.sum(grad_f32 * x_hat, axis=(0, 1))
    grad_hat = grad_f32 * norm_gain.astype(jnp.float32)
    grad_in = inv_rms * (grad_hat - x_hat * jnp.mean(grad_hat * x_hat, axis=-1, keepdims=True))
    grad_rows = grad_in.astype(jnp.bfloat16).astype(jnp.float32).reshape(-1, HIDDEN)
    grad_table = jax.ops.segment_sum(grad_rows, token_ids.reshape(-1), num_segments=VOCAB_SIZE)
    return normed, grad_table, grad_gain
```

```python
import functools

import jax
import jax.numpy as jnp
from jax import lax
from jax.experimental import pallas as pl
from jax.experimental.pallas import tpu as pltpu
from jax.sharding import PartitionSpec as P

RMS_EPS = 1e-5
TP = 16
ROWS = 3072
HID = 2048
SEQ = 2048
TOK = 128
XC = 32
DC = 64
NC = 512
CHUNKS = 6
MESH = pl.DeviceIdType.MESH
F32 = jnp.float32
BF16 = jnp.bfloat16
I32 = jnp.int32


def dot(a, b):
    return lax.dot_general(a, b, (((1,), (0,)), ((), ())), preferred_element_type=F32)


def one_hot(mask):
    return jnp.where(mask, 1.0, 0.0).astype(BF16)


def owner_of(ids):
    return ((ids >> 10) * 171) >> 9


def columns(rows):
    pad = jnp.zeros((128 - rows.shape[0], 128), rows.dtype)
    return jnp.concatenate([rows, pad], axis=0).T


def exchange_kernel(
    ids_ref, table_ref, gain_ref, grad_ref,
    dxc_ref, clid_ref, ys_ref, ydst_ref, dgp_ref, flag_ref,
    tbl, tbl_sem, xs, xrecv, ds, drecv, dgs, xid_s,
    xz_send, xf_send, x_sem, dz_send, df_send, d_sem, g_send, g_sem,
):
    me = lax.axis_index('tp')
    z = me // 4
    lane = me % 4
    y = lane // 2
    c = lane % 2
    sib = z * 4 + y * 2 + (1 - c)
    ymate = z * 4 + (1 - y) * 2 + c
    far = z * 4 + (1 - y) * 2 + (1 - c)
    zs = [z, z + 1 - 2 * (z % 2), z + 2 - 4 * (z // 2), 3 - z]

    barrier = pltpu.get_barrier_semaphore()

    def greet(i, carry):
        pl.semaphore_signal(barrier, inc=1, device_id={'tp': (me + i) % TP}, device_id_type=MESH)
        return carry

    lax.fori_loop(1, TP, greet, 0)

    part = ROWS // CHUNKS
    loads = [
        pltpu.make_async_copy(table_ref.at[pl.ds(i * part, part)], tbl.at[pl.ds(i * part, part)], tbl_sem.at[i])
        for i in range(CHUNKS)
    ]
    for load in loads:
        load.start()

    ids = ids_ref[...]
    own = owner_of(ids)
    idc = columns(ids)
    sub = lax.broadcasted_iota(I32, (128, 128), 0)
    lan = lax.broadcasted_iota(I32, (128, 128), 1)
    before = sub < lan
    dup_rows = []
    for s in range(4):
        for b in range(4):
            acc = jnp.zeros((128, 128), I32)
            row = ids[4 * s + b:4 * s + b + 1, :]
            for a in range(b + 1):
                same = idc[:, 4 * s + a:4 * s + a + 1] == row
                if a == b:
                    same = same & before
                acc = acc | jnp.where(same, 1, 0)
            dup_rows.append(jnp.max(acc, axis=0, keepdims=True))
    first = jnp.concatenate(dup_rows, axis=0) == 0
    key = jnp.where(first, own, -1)
    keyc = columns(key)
    rank_rows = []
    for s in range(4):
        for b in range(4):
            acc = jnp.zeros((128, 128), I32)
            row = own[4 * s + b:4 * s + b + 1, :]
            for a in range(b + 1):
                same = keyc[:, 4 * s + a:4 * s + a + 1] == row
                if a == b:
                    same = same & before
                acc = acc + jnp.where(same, 1, 0)
            rank_rows.append(jnp.sum(acc, axis=0, keepdims=True))
    rank = jnp.concatenate(rank_rows, axis=0)

    local = ids - me * ROWS
    mine = own == me
    xslot = jnp.where(first & mine, rank, -1)
    slot_iota = lax.broadcasted_iota(I32, (XC, 128), 0)
    lids = []
    for s in range(4):
        acc = jnp.zeros((XC, 128), I32)
        for a in range(4):
            d = 4 * s + a
            acc = acc + jnp.where(slot_iota == xslot[d:d + 1, :], local[d:d + 1, :] + 1, 0)
        lids.append(jnp.sum(acc, axis=1, keepdims=True) - 1)
    lid = jnp.concatenate(lids, axis=0)

    packed = jnp.zeros((4 * XC, HID), F32)
    chunk_iota = lax.broadcasted_iota(I32, (4 * XC, part), 1)
    for i in range(CHUNKS):
        loads[i].wait()
        packed = packed + dot(one_hot(chunk_iota + i * part == lid), tbl[pl.ds(i * part, part), :])
    packed = packed.astype(BF16)
    for s in range(4):
        xs[s] = packed[s * XC:(s + 1) * XC, :]
    xrecv[me] = xs[z]

    pl.semaphore_wait(barrier, TP - 1)

    def send(src, dst, ssem, rsem, dev):
        cp = pltpu.make_async_remote_copy(
            src_ref=src, dst_ref=dst, send_sem=ssem, recv_sem=rsem, device_id={'tp': dev}, device_id_type=MESH)
        cp.start()
        return cp

    sends = []

    def arrive(buf, sem, src):
        pltpu.make_async_remote_copy(
            src_ref=buf.at[src], dst_ref=buf.at[src], send_sem=xz_send.at[0], recv_sem=sem.at[src],
            device_id={'tp': sib}, device_id_type=MESH).wait_recv()

    def forward_own(buf, ssem, sem, k):
        src = zs[k] * 4 + lane
        if k:
            arrive(buf, sem, src)
        sends.append(send(buf.at[src], buf.at[src], ssem.at[3 * k], sem.at[src], ymate))
        sends.append(send(buf.at[src], buf.at[src], ssem.at[3 * k + 1], sem.at[src], sib))

    def forward_mate(buf, ssem, sem, k):
        src = zs[k] * 4 + (1 - y) * 2 + c
        arrive(buf, sem, src)
        sends.append(send(buf.at[src], buf.at[src], ssem.at[3 * k + 2], sem.at[src], sib))

    def collect(buf, sem, k):
        arrive(buf, sem, zs[k] * 4 + y * 2 + (1 - c))
        arrive(buf, sem, zs[k] * 4 + (1 - y) * 2 + (1 - c))

    for k in range(1, 4):
        sends.append(send(xs.at[zs[k]], xrecv.at[me], xz_send.at[k - 1], x_sem.at[me], zs[k] * 4 + lane))
    forward_own(xrecv, xf_send, x_sem, 0)

    xall = jnp.where(first, own * XC + rank, -1)
    over = jnp.max(jnp.where(first & (rank >= XC), 1, 0))

    def slab(rows):
        out = jnp.zeros((4, 128), I32)
        for s in range(4):
            out = out + jnp.where(z == s, rows[4 * s:4 * s + 4, :], 0)
        return out

    tslot = jnp.where(slab(jnp.where(first, 1, 0)) == 1, slab(jnp.where(rank < XC, xall, -1)), -1)
    mine_c = columns(jnp.concatenate([tslot, slab(ids)], axis=0))
    for q in range(4):
        acc = jnp.zeros((128, 128), I32)
        for a in range(4):
            acc = acc + jnp.where(mine_c[:, a:a + 1] == lan + q * 128, mine_c[:, 4 + a:5 + a] + 1, 0)
        xid_s[q:q + 1, :] = jnp.sum(acc, axis=0, keepdims=True) - 1

    zown = own >> 2
    zc = ((idc >> 10) * 171) >> 11
    drank_rows = []
    for d in range(TP):
        same = (zc[:, d:d + 1] == zown[d:d + 1, :]) & before
        drank_rows.append(jnp.sum(jnp.where(same, 1, 0), axis=0, keepdims=True))
    drank = jnp.concatenate(drank_rows, axis=0)
    over = jnp.maximum(over, jnp.max(jnp.where(drank >= DC, 1, 0)))
    row_iota = lax.broadcasted_iota(I32, (TP, 128), 0)

    def my_row(rows):
        return jnp.sum(jnp.where(row_iota == me, rows, 0), axis=0, keepdims=True)

    my_ids, my_rank, my_zown = my_row(ids), my_row(drank), my_row(zown)
    ydst_ref[...] = jnp.broadcast_to(my_zown * DC + my_rank, (8, 128))
    dslot_iota = lax.broadcasted_iota(I32, (DC, 128), 0)
    gain = gain_ref[...]
    gain_f = gain.astype(F32)
    gain_sum = jnp.zeros((1, HID), F32)

    forward_mate(xrecv, xf_send, x_sem, 0)
    for k in range(4):
        if k < 3:
            forward_own(xrecv, xf_send, x_sem, k + 1)
        collect(xrecv, x_sem, k)
        zk = zs[k]
        pick = (dslot_iota == my_rank) & (my_zown == zk)
        did = jnp.sum(jnp.where(pick, my_ids + 1, 0), axis=1, keepdims=True) - 1
        xid = xid_s[pl.ds(zk, 1), :]
        from_recv = one_hot((did == xid) & (did >= 0))
        h_all = dot(from_recv, jnp.concatenate([xrecv[zk * 4 + j] for j in range(4)], axis=0))
        g_all = dot(one_hot(pick), grad_ref[...])
        dst = me if k == 0 else zk
        for r0 in range(0, DC, 16):
            h = h_all[r0:r0 + 16, :]
            inv = lax.rsqrt(jnp.mean(h * h, axis=-1, keepdims=True) + RMS_EPS)
            xh = h * inv
            gr = g_all[r0:r0 + 16, :]
            gain_sum = gain_sum + jnp.sum(gr * xh, axis=0, keepdims=True)
            u = gr * gain_f
            dx = inv * (u - xh * jnp.mean(u * xh, axis=-1, keepdims=True))
            ys_ref[zk, pl.ds(r0, 16), :] = xh.astype(BF16) * gain
            if k == 0:
                drecv[me, pl.ds(r0, 16), :] = dx.astype(BF16)
            else:
                ds[k - 1, pl.ds(r0, 16), :] = dx.astype(BF16)
        if k:
            sends.append(send(ds.at[k - 1], drecv.at[me], dz_send.at[k - 1], d_sem.at[me], zk * 4 + lane))
        else:
            forward_own(drecv, df_send, d_sem, 0)
        if k < 3:
            forward_mate(xrecv, xf_send, x_sem, k + 1)
        else:
            forward_mate(drecv, df_send, d_sem, 0)

    dgs[...] = gain_sum
    dgp_ref[me] = gain_sum
    for i in range(1, TP):
        sends.append(send(dgs, dgp_ref.at[me], g_send.at[i - 1], g_sem.at[me], (me + i) % TP))

    dslot = jnp.where(mine & (drank < DC), drank, -1)
    dslot_c = columns(dslot)
    lrows = []
    for p in range(8):
        acc = jnp.zeros((128, 128), I32)
        for j in range(2):
            d = 2 * p + j
            sc = dslot_c[:, d:d + 1]
            acc = acc + jnp.where((sc >= 0) & (sc + 64 * j == lan), idc[:, d:d + 1] - me * ROWS + 1, 0)
        lrows.append(jnp.sum(acc, axis=0, keepdims=True))
    lid1 = jnp.concatenate(lrows, axis=0)
    has = lid1 > 0
    has_f = jnp.where(has, 1.0, 0.0)
    inrow = dot(has_f.astype(BF16), one_hot(before))
    total = jnp.sum(has_f, axis=1, keepdims=True)
    crank_rows = []
    base = jnp.zeros((1, 1), F32)
    for p in range(8):
        crank_rows.append(inrow[p:p + 1, :] + base)
        base = base + total[p:p + 1, :]
    for o in range(TP):
        over = jnp.maximum(over, jnp.where(jnp.sum(jnp.where(own == o, 1.0, 0.0)) > NC, 1, 0))
    crank = jnp.where(has, jnp.concatenate(crank_rows, axis=0).astype(I32), -1)
    n_iota = lax.broadcasted_iota(I32, (NC, 128), 0)
    compact = jnp.concatenate([one_hot(n_iota == crank[p:p + 1, :]) for p in range(8)], axis=1)
    lrow = jnp.concatenate([lid1[p:p + 1, :] for p in range(8)], axis=1)
    halves = jnp.concatenate([lrow >> 6, lrow & 63, jnp.zeros((6, TP * DC), I32)], axis=0).astype(F32).astype(BF16)
    cl = lax.dot_general(halves, compact, (((1,), (1,)), ((), ())), preferred_element_type=F32)
    clid_ref[...] = jnp.broadcast_to((cl[0:1, :] * 64.0 + cl[1:2, :]).astype(I32) - 1, (8, NC))
    flag_ref[0] = over

    for k in range(1, 4):
        forward_own(drecv, df_send, d_sem, k)
        forward_mate(drecv, df_send, d_sem, k)
    for k in range(4):
        collect(drecv, d_sem, k)
    dxc_ref[...] = dot(compact, jnp.concatenate([drecv[d] for d in range(TP)], axis=0)).astype(BF16)
    for i in range(1, TP):
        src = (me + i) % TP
        pltpu.make_async_remote_copy(
            src_ref=dgs, dst_ref=dgp_ref.at[src], send_sem=g_send.at[i - 1], recv_sem=g_sem.at[src],
            device_id={'tp': sib}, device_id_type=MESH).wait_recv()
    for cp in sends:
        cp.wait_send()


def exchange(ids, table, gain, grad):
    vmem = pl.BlockSpec(memory_space=pltpu.VMEM)
    return pl.pallas_call(
        exchange_kernel,
        out_shape=(
            jax.ShapeDtypeStruct((NC, HID), BF16),
            jax.ShapeDtypeStruct((8, NC), I32),
            jax.ShapeDtypeStruct((4, DC, HID), BF16),
            jax.ShapeDtypeStruct((8, 128), I32),
            jax.ShapeDtypeStruct((TP, 1, HID), F32),
            jax.ShapeDtypeStruct((1,), I32),
        ),
        in_specs=[vmem, pl.BlockSpec(memory_space=pl.ANY), vmem, vmem],
        out_specs=(vmem, vmem, vmem, vmem, vmem, pl.BlockSpec(memory_space=pltpu.SMEM)),
        scratch_shapes=[
            pltpu.VMEM((ROWS, HID), BF16),
            pltpu.SemaphoreType.DMA((CHUNKS,)),
            pltpu.VMEM((4, XC, HID), BF16),
            pltpu.VMEM((TP, XC, HID), BF16),
            pltpu.VMEM((3, DC, HID), BF16),
            pltpu.VMEM((TP, DC, HID), BF16),
            pltpu.VMEM((1, HID), F32),
            pltpu.VMEM((8, 128), I32),
            pltpu.SemaphoreType.DMA((3,)),
            pltpu.SemaphoreType.DMA((12,)),
            pltpu.SemaphoreType.DMA((TP,)),
            pltpu.SemaphoreType.DMA((3,)),
            pltpu.SemaphoreType.DMA((12,)),
            pltpu.SemaphoreType.DMA((TP,)),
            pltpu.SemaphoreType.DMA((TP - 1,)),
            pltpu.SemaphoreType.DMA((TP,)),
        ],
        compiler_params=pltpu.CompilerParams(collective_id=0, has_side_effects=True),
        name='exchange',
    )(ids, table, gain, grad)


BLK = 128


def finish_kernel(dxc_ref, clid_ref, ys_ref, ydst_ref, dgp_ref, de_ref, y_ref, dg_ref):
    i = pl.program_id(0)
    rows = lax.broadcasted_iota(I32, (BLK, NC), 0) + i * BLK
    de_ref[...] = dot(one_hot(rows == clid_ref[0:1, :]), dxc_ref[...])

    @pl.when(i == 0)
    def _():
        spread = one_hot(lax.broadcasted_iota(I32, (4 * DC, 128), 0) == ydst_ref[0:1, :])
        ys = jnp.concatenate([ys_ref[s] for s in range(4)], axis=0)
        y_ref[...] = lax.dot_general(spread, ys, (((0,), (0,)), ((), ())), preferred_element_type=F32).astype(BF16)
        total = dgp_ref[0]
        for d in range(1, TP):
            total = total + dgp_ref[d]
        dg_ref[...] = total


def finish(dxc, clid, ys, ydst, dgp):
    def whole(shape):
        return pl.BlockSpec(shape, lambda i: (0,) * len(shape))

    return pl.pallas_call(
        finish_kernel,
        grid=(ROWS // BLK,),
        out_shape=(
            jax.ShapeDtypeStruct((ROWS, HID), F32),
            jax.ShapeDtypeStruct((TOK, HID), BF16),
            jax.ShapeDtypeStruct((1, HID), F32),
        ),
        in_specs=[whole((NC, HID)), whole((8, NC)), whole((4, DC, HID)), whole((8, 128)), whole((TP, 1, HID))],
        out_specs=(pl.BlockSpec((BLK, HID), lambda i: (i, 0)), whole((TOK, HID)), whole((1, HID))),
        name='finish',
    )(dxc, clid, ys, ydst, dgp)


def swap_kernel(src_ref, dst_ref, local_sem, send_sem, recv_sem):
    me = lax.axis_index('tp')
    barrier = pltpu.get_barrier_semaphore()

    def greet(i, carry):
        pl.semaphore_signal(barrier, inc=1, device_id={'tp': (me + i) % TP}, device_id_type=MESH)
        return carry

    lax.fori_loop(1, TP, greet, 0)
    pl.semaphore_wait(barrier, TP - 1)

    def copy(i):
        peer = (me + i) % TP
        return pltpu.make_async_remote_copy(
            src_ref=src_ref.at[peer], dst_ref=dst_ref.at[me], send_sem=send_sem.at[i], recv_sem=recv_sem.at[me],
            device_id={'tp': peer}, device_id_type=MESH)

    def start(i, carry):
        copy(i).start()
        return carry

    lax.fori_loop(1, TP, start, 0)
    keep = pltpu.make_async_copy(src_ref.at[me], dst_ref.at[me], local_sem)
    keep.start()

    def wait(i, carry):
        peer = (me + i) % TP
        pltpu.make_async_remote_copy(
            src_ref=src_ref.at[peer], dst_ref=dst_ref.at[peer], send_sem=send_sem.at[i], recv_sem=recv_sem.at[peer],
            device_id={'tp': peer}, device_id_type=MESH).wait()
        return carry

    lax.fori_loop(1, TP, wait, 0)
    keep.wait()


def swap(blocks, cid):
    return pl.pallas_call(
        swap_kernel,
        out_shape=jax.ShapeDtypeStruct(blocks.shape, blocks.dtype),
        in_specs=[pl.BlockSpec(memory_space=pl.ANY)],
        out_specs=pl.BlockSpec(memory_space=pl.ANY),
        scratch_shapes=[pltpu.SemaphoreType.DMA, pltpu.SemaphoreType.DMA((TP,)), pltpu.SemaphoreType.DMA((TP,))],
        compiler_params=pltpu.CompilerParams(collective_id=cid, has_side_effects=True),
        name='swap',
    )(blocks)


def general(ids, table, gain, grad):
    local = ids.reshape(-1) - lax.axis_index('tp') * ROWS
    mine = (local >= 0) & (local < ROWS)
    looked = jnp.take(table, jnp.where(mine, local, 0), axis=0)
    parts = swap(jnp.where(mine[:, None], looked, jnp.zeros((), BF16)).reshape(TP, TOK, HID), 1)
    h = jnp.sum(parts.astype(F32), axis=0)
    inv = lax.rsqrt(jnp.mean(h * h, axis=-1, keepdims=True) + RMS_EPS)
    xh = h * inv
    y = xh.astype(BF16) * gain
    gr = grad.astype(F32)
    part = jnp.sum(gr * xh, axis=0)
    u = gr * gain.astype(F32)
    dx = (inv * (u - xh * jnp.mean(u * xh, axis=-1, keepdims=True))).astype(BF16)
    dx_all = swap(jnp.broadcast_to(dx[None], (TP, TOK, HID)), 2).reshape(SEQ, HID)
    dg = jnp.sum(swap(jnp.broadcast_to(part.reshape(1, TOK // 8, 128), (TP, TOK // 8, 128)), 3), axis=0).reshape(1, HID)
    de = jax.ops.segment_sum(dx_all.astype(F32), jnp.where(mine, local, ROWS), num_segments=ROWS)
    return de, y, dg


def device_step(token_ids, table, gain, grad):
    ids = token_ids.reshape(TP, TOK)
    gain = gain.reshape(1, HID)
    grad = grad.reshape(TOK, HID)
    dxc, clid, ys, ydst, dgp, flag = exchange(ids, table, gain, grad)
    de, y, dg = lax.cond(
        flag[0] > 0,
        lambda: general(ids, table, gain, grad),
        lambda: finish(dxc, clid, ys, ydst, dgp),
    )
    return y.reshape(1, TOK, HID), de, dg.reshape(HID)


def solution(mesh):
    return jax.shard_map(
        device_step, mesh=mesh,
        in_specs=(P('dp', None), P('tp', None), P(None), P('dp', 'tp', None)),
        out_specs=(P('dp', 'tp', None), P(('dp', 'tp'), None), P('dp')), check_vma=False)
```

```python
import functools

import jax
import jax.numpy as jnp
from jax import lax
from jax.experimental import pallas as pl
from jax.experimental.pallas import tpu as pltpu
from jax.sharding import PartitionSpec as P

RMS_EPS = 1e-5
TP = 16
ROWS = 3072
HID = 2048
SEQ = 2048
TOK = 128
XC = 32
DC = 56
DW = 40
NC = 512
CHUNKS = 6
MESH = pl.DeviceIdType.MESH
F32 = jnp.float32
BF16 = jnp.bfloat16
I32 = jnp.int32


def dot(a, b):
    return lax.dot_general(a, b, (((1,), (0,)), ((), ())), preferred_element_type=F32)


def one_hot(mask):
    return jnp.where(mask, 1.0, 0.0).astype(BF16)


def owner_of(ids):
    return ((ids >> 10) * 171) >> 9


def columns(rows):
    pad = jnp.zeros((128 - rows.shape[0], 128), rows.dtype)
    return jnp.concatenate([rows, pad], axis=0).T


def exchange_kernel(
    ids_ref, table_ref, gain_ref, grad_ref,
    dxc_ref, clid_ref, y_ref, dgp_ref, flag_ref,
    tbl, tbl_sem, xs, xrecv, ds, zbuf, drecv, dxs, dgs,
    xz_send, xf_send, x_sem, dz_send, z_sem, df_send, d_sem, g_send, g_sem,
):
    me = lax.axis_index('tp')
    z = me // 4
    lane = me % 4
    y = lane // 2
    c = lane % 2
    sib = z * 4 + y * 2 + (1 - c)
    ymate = z * 4 + (1 - y) * 2 + c
    zs = [z, z + 1 - 2 * (z % 2), z + 2 - 4 * (z // 2), 3 - z]

    barrier = pltpu.get_barrier_semaphore()

    def greet(i, carry):
        pl.semaphore_signal(barrier, inc=1, device_id={'tp': (me + i) % TP}, device_id_type=MESH)
        return carry

    lax.fori_loop(1, TP, greet, 0)

    part = ROWS // CHUNKS
    loads = [
        pltpu.make_async_copy(table_ref.at[pl.ds(i * part, part)], tbl.at[pl.ds(i * part, part)], tbl_sem.at[i])
        for i in range(CHUNKS)
    ]
    for load in loads:
        load.start()

    sends = []

    def send(src, dst, ssem, rsem, dev):
        cp = pltpu.make_async_remote_copy(
            src_ref=src, dst_ref=dst, send_sem=ssem, recv_sem=rsem, device_id={'tp': dev}, device_id_type=MESH)
        cp.start()
        sends.append(cp)

    def arrived(ref, sem):
        pltpu.make_async_remote_copy(
            src_ref=ref, dst_ref=ref, send_sem=xz_send.at[0], recv_sem=sem,
            device_id={'tp': sib}, device_id_type=MESH).wait_recv()

    ids = ids_ref[...]
    own = owner_of(ids)
    row_iota = lax.broadcasted_iota(I32, (TP, 128), 0)
    sub = lax.broadcasted_iota(I32, (128, 128), 0)
    lan = lax.broadcasted_iota(I32, (128, 128), 1)
    before = sub < lan

    def my_row(rows):
        return jnp.sum(jnp.where(row_iota == me, rows, 0), axis=0, keepdims=True)

    my_own = my_row(own)
    my_own_c = columns(jnp.broadcast_to(my_own, (8, 128)))[:, 0:1]
    my_chip = my_own >> 1
    same = ((my_own_c >> 1) == my_chip) & before
    my_rank = jnp.sum(jnp.where(same, 1, 0), axis=0, keepdims=True)
    my_slot = jnp.where((my_chip & 1) == 0, my_rank, DC - 1 - my_rank)
    my_zown = my_own >> 2
    dslot_iota = lax.broadcasted_iota(I32, (DC, 128), 0)

    def pack_dy(k):
        pick = (dslot_iota == my_slot) & (my_zown == zs[k])
        return dot(one_hot(pick), grad_ref[...]).astype(BF16)

    lo, hi = y * (DC - DW), (1 - y) * (DC - DW)

    def forward_z(k):
        src = zs[k] * 4 + lane
        if k:
            arrived(zbuf.at[k], z_sem.at[k])
        send(zbuf.at[k, pl.ds(pl.multiple_of(hi, 8), DW)], drecv.at[src], df_send.at[3 * k], d_sem.at[src], ymate)
        send(zbuf.at[k, pl.ds(pl.multiple_of(lo, 8), DW)], drecv.at[src], df_send.at[3 * k + 1], d_sem.at[src], sib)

    def forward_zmate(k):
        src = zs[k] * 4 + (1 - y) * 2 + c
        arrived(drecv.at[src], d_sem.at[src])
        send(drecv.at[src], drecv.at[src], df_send.at[3 * k + 2], d_sem.at[src], sib)

    def collect_dy(k):
        for j in range(2):
            src = zs[k] * 4 + ((1 - y) * 2 if j else y * 2) + (1 - c)
            arrived(drecv.at[src], d_sem.at[src])

    for k in (1, 2, 3):
        ds[k - 1] = pack_dy(k)
    zbuf[0] = pack_dy(0)
    pl.semaphore_wait(barrier, TP - 1)
    for k in (1, 2, 3):
        send(ds.at[k - 1], zbuf.at[k], dz_send.at[k - 1], z_sem.at[k], zs[k] * 4 + lane)
    forward_z(0)

    idc = columns(ids)
    dup_rows = []
    for s in range(4):
        for b in range(4):
            acc = jnp.zeros((128, 128), I32)
            row = ids[4 * s + b:4 * s + b + 1, :]
            for a in range(b + 1):
                same = idc[:, 4 * s + a:4 * s + a + 1] == row
                if a == b:
                    same = same & before
                acc = acc | jnp.where(same, 1, 0)
            dup_rows.append(jnp.max(acc, axis=0, keepdims=True))
    first = jnp.concatenate(dup_rows, axis=0) == 0
    key = jnp.where(first, own, -1)
    keyc = columns(key)
    rank_rows = []
    for s in range(4):
        for b in range(4):
            acc = jnp.zeros((128, 128), I32)
            row = own[4 * s + b:4 * s + b + 1, :]
            for a in range(b + 1):
                same = keyc[:, 4 * s + a:4 * s + a + 1] == row
                if a == b:
                    same = same & before
                acc = acc + jnp.where(same, 1, 0)
            rank_rows.append(jnp.sum(acc, axis=0, keepdims=True))
    rank = jnp.concatenate(rank_rows, axis=0)

    local = ids - me * ROWS
    mine = own == me
    xslot = jnp.where(first & mine, rank, -1)
    slot_iota = lax.broadcasted_iota(I32, (XC, 128), 0)
    lids = []
    for s in range(4):
        acc = jnp.zeros((XC, 128), I32)
        for a in range(4):
            d = 4 * s + a
            acc = acc + jnp.where(slot_iota == xslot[d:d + 1, :], local[d:d + 1, :] + 1, 0)
        lids.append(jnp.sum(acc, axis=1, keepdims=True) - 1)
    lid = jnp.concatenate(lids, axis=0)

    packed = jnp.zeros((4 * XC, HID), F32)
    chunk_iota = lax.broadcasted_iota(I32, (4 * XC, part), 1)
    for i in range(CHUNKS):
        loads[i].wait()
        packed = packed + dot(one_hot(chunk_iota + i * part == lid), tbl[pl.ds(i * part, part), :])
    packed = packed.astype(BF16)
    for s in range(4):
        xs[s] = packed[s * XC:(s + 1) * XC, :]
    xrecv[me] = xs[z]

    def forward_x(k):
        src = zs[k] * 4 + lane
        if k:
            arrived(xrecv.at[src], x_sem.at[src])
        send(xrecv.at[src], xrecv.at[src], xf_send.at[3 * k], x_sem.at[src], ymate)
        send(xrecv.at[src], xrecv.at[src], xf_send.at[3 * k + 1], x_sem.at[src], sib)

    def forward_xmate(k):
        src = zs[k] * 4 + (1 - y) * 2 + c
        arrived(xrecv.at[src], x_sem.at[src])
        send(xrecv.at[src], xrecv.at[src], xf_send.at[3 * k + 2], x_sem.at[src], sib)

    def collect_x(k):
        for j in range(2):
            src = zs[k] * 4 + ((1 - y) * 2 if j else y * 2) + (1 - c)
            arrived(xrecv.at[src], x_sem.at[src])

    for k in (1, 2, 3):
        send(xs.at[zs[k]], xrecv.at[me], xz_send.at[k - 1], x_sem.at[me], zs[k] * 4 + lane)
    forward_x(0)
    forward_z(1)
    forward_zmate(0)

    over = jnp.max(jnp.where(first & (rank >= XC), 1, 0))

    def slab(rows):
        out = jnp.zeros((4, 128), I32)
        for s in range(4):
            out = out + jnp.where(z == s, rows[4 * s:4 * s + 4, :], 0)
        return out

    tslot = slab(jnp.where(first & (rank < XC), own * XC + rank, -1))
    mine_c = columns(jnp.concatenate([tslot, slab(ids), jnp.broadcast_to(my_row(ids), (8, 128))], axis=0))
    my_ids_c = mine_c[:, 8:9]
    spread = []
    for q in range(4):
        acc = jnp.zeros((128, 128), I32)
        for a in range(4):
            acc = acc + jnp.where(mine_c[:, a:a + 1] == lan + q * 128, mine_c[:, 4 + a:5 + a] + 1, 0)
        spread.append(one_hot(my_ids_c == jnp.sum(acc, axis=0, keepdims=True) - 1))
    spread = jnp.concatenate(spread, axis=1)

    chip_c = ((idc >> 10) * 171) >> 10
    chip = own >> 1
    drank_rows = []
    for d in range(TP):
        same = (chip_c[:, d:d + 1] == chip[d:d + 1, :]) & before
        drank_rows.append(jnp.sum(jnp.where(same, 1, 0), axis=0, keepdims=True))
    drank = jnp.concatenate(drank_rows, axis=0)
    over = jnp.maximum(over, jnp.max(jnp.where(drank >= DW, 1, 0)))
    for s in range(4):
        in_slab = jnp.sum(jnp.where((own >> 2) == s, 1.0, 0.0), axis=1, keepdims=True)
        over = jnp.maximum(over, jnp.max(jnp.where(in_slab > DC, 1, 0)))
    for o in range(TP):
        over = jnp.maximum(over, jnp.where(jnp.sum(jnp.where(own == o, 1.0, 0.0)) > NC, 1, 0))
    flag_ref[0] = over
    forward_xmate(0)

    dslot = jnp.where(mine & (drank < DW), jnp.where(y == 0, drank, DW - 1 - drank), -1)
    dslot_c = columns(dslot)
    lrows = []
    for p in range(TP * DW // 128):
        acc = jnp.zeros((128, 128), I32)
        for d in range(TP):
            if d * DW < (p + 1) * 128 and (d + 1) * DW > p * 128:
                sc = dslot_c[:, d:d + 1]
                acc = acc + jnp.where((sc >= 0) & (sc + (d * DW - p * 128) == lan), idc[:, d:d + 1] - me * ROWS + 1, 0)
        lrows.append(jnp.sum(acc, axis=0, keepdims=True))
    lid1 = jnp.concatenate(lrows + [jnp.zeros((8 - len(lrows), 128), I32)], axis=0)
    has = lid1 > 0
    has_f = jnp.where(has, 1.0, 0.0)
    inrow = dot(has_f.astype(BF16), one_hot(before))
    total = jnp.sum(has_f, axis=1, keepdims=True)
    crank_rows = []
    base = jnp.zeros((1, 1), F32)
    for p in range(8):
        crank_rows.append(inrow[p:p + 1, :] + base)
        base = base + total[p:p + 1, :]
    crank = jnp.where(has, jnp.concatenate(crank_rows, axis=0).astype(I32), -1)
    n_iota = lax.broadcasted_iota(I32, (NC, 128), 0)
    compact = jnp.concatenate([one_hot(n_iota == crank[p:p + 1, :]) for p in range(len(lrows))], axis=1)
    lrow = jnp.concatenate([lid1[p:p + 1, :] for p in range(len(lrows))], axis=1)
    halves = jnp.concatenate([lrow >> 6, lrow & 63, jnp.zeros((6, TP * DW), I32)], axis=0).astype(F32).astype(BF16)
    cl = lax.dot_general(halves, compact, (((1,), (1,)), ((), ())), preferred_element_type=F32)
    clid_ref[...] = jnp.broadcast_to((cl[0:1, :] * 64.0 + cl[1:2, :]).astype(I32) - 1, (8, NC))

    gain = gain_ref[...]
    gain_f = gain.astype(F32)
    xlid = jnp.broadcast_to(lid, (4 * XC, 128)).T[0:1, :]
    w_iota = lax.broadcasted_iota(I32, (DW, 128), 0)
    x_group = lax.broadcasted_iota(I32, (1, 4 * XC), 1) // XC

    steps = [(r0, min(16, DW - r0)) for r0 in range(0, DW, 16)]

    def dx_rows(zk, dy_of, gain_sum):
        pick_row = jnp.where(x_group == zk, xlid, -2)
        for block, at in dy_of:
            slot_row = jnp.sum(jnp.where(row_iota == at, dslot, 0), axis=0, keepdims=True)
            local_row = jnp.sum(jnp.where(row_iota == at, local, 0), axis=0, keepdims=True)
            dlid = jnp.sum(jnp.where(w_iota == slot_row, local_row + 1, 0), axis=1, keepdims=True) - 1
            h_all = dot(one_hot(dlid == pick_row), jnp.concatenate([xs[s] for s in range(4)], axis=0))
            for r0, n in steps:
                h = h_all[r0:r0 + n, :]
                inv = lax.rsqrt(jnp.mean(h * h, axis=-1, keepdims=True) + RMS_EPS)
                xh = h * inv
                gr = block(r0, n).astype(F32)
                gain_sum = gain_sum + jnp.sum(gr * xh, axis=0, keepdims=True)
                u = gr * gain_f
                dx = inv * (u - xh * jnp.mean(u * xh, axis=-1, keepdims=True))
                dxs[at, pl.ds(r0, n), :] = dx.astype(BF16)
        return gain_sum

    def process(k, gain_sum):
        collect_dy(k)
        zk = zs[k]
        out = [(lambda r0, n: zbuf[k, pl.ds(pl.multiple_of(lo + r0, 8), n), :], zk * 4 + lane)]
        for off in ((1 - y) * 2 + c, y * 2 + (1 - c), (1 - y) * 2 + (1 - c)):
            at = zk * 4 + off
            out.append((lambda r0, n, at=at: drecv[at, pl.ds(r0, n), :], at))
        return dx_rows(zk, out, gain_sum)

    forward_z(2)
    forward_zmate(1)
    gain_sum = process(0, jnp.zeros((1, HID), F32))
    forward_z(3)
    forward_zmate(2)
    gain_sum = process(1, gain_sum)
    forward_x(1)
    forward_zmate(3)
    gain_sum = process(2, gain_sum)
    forward_x(2)
    forward_xmate(1)
    gain_sum = process(3, gain_sum)
    dgs[...] = gain_sum
    dgp_ref[me] = gain_sum
    for i in range(1, TP):
        send(dgs, dgp_ref.at[me], g_send.at[i - 1], g_sem.at[me], (me + i) % TP)
    forward_x(3)
    forward_xmate(2)
    dxc_ref[...] = dot(compact, jnp.concatenate([dxs[d] for d in range(TP)], axis=0)).astype(BF16)
    forward_xmate(3)
    for k in range(4):
        collect_x(k)
    h_all = dot(spread, jnp.concatenate([xrecv[d] for d in range(TP)], axis=0))
    for r0 in range(0, TOK, 16):
        h = h_all[r0:r0 + 16, :]
        xh = h * lax.rsqrt(jnp.mean(h * h, axis=-1, keepdims=True) + RMS_EPS)
        y_ref[pl.ds(r0, 16), :] = xh.astype(BF16) * gain
    for i in range(1, TP):
        src = (me + i) % TP
        arrived(dgp_ref.at[src], g_sem.at[src])
    for cp in sends:
        cp.wait_send()


def exchange(ids, table, gain, grad):
    vmem = pl.BlockSpec(memory_space=pltpu.VMEM)
    dma = pltpu.SemaphoreType.DMA
    return pl.pallas_call(
        exchange_kernel,
        out_shape=(
            jax.ShapeDtypeStruct((NC, HID), BF16),
            jax.ShapeDtypeStruct((8, NC), I32),
            jax.ShapeDtypeStruct((TOK, HID), BF16),
            jax.ShapeDtypeStruct((TP, 1, HID), F32),
            jax.ShapeDtypeStruct((1,), I32),
        ),
        in_specs=[vmem, pl.BlockSpec(memory_space=pltpu.HBM), vmem, vmem],
        out_specs=(vmem, vmem, vmem, vmem, pl.BlockSpec(memory_space=pltpu.SMEM)),
        scratch_shapes=[
            pltpu.VMEM((ROWS, HID), BF16),
            dma((CHUNKS,)),
            pltpu.VMEM((4, XC, HID), BF16),
            pltpu.VMEM((TP, XC, HID), BF16),
            pltpu.VMEM((3, DC, HID), BF16),
            pltpu.VMEM((4, DC, HID), BF16),
            pltpu.VMEM((TP, DW, HID), BF16),
            pltpu.VMEM((TP, DW, HID), BF16),
            pltpu.VMEM((1, HID), F32),
            dma((3,)), dma((12,)), dma((TP,)), dma((3,)), dma((4,)), dma((12,)), dma((TP,)), dma((TP - 1,)), dma((TP,)),
        ],
        compiler_params=pltpu.CompilerParams(collective_id=0, has_side_effects=True),
        name='exchange',
    )(ids, table, gain, grad)


BLK = 512
HALF = NC // 2


def finish_kernel(dxc_ref, clid_ref, y_in_ref, dgp_ref, de_ref, y_ref, dg_ref, sem):
    i = pl.program_id(0)
    keep = pltpu.make_async_copy(y_in_ref, y_ref, sem)

    @pl.when(i == 0)
    def _():
        keep.start()

    rows = lax.broadcasted_iota(I32, (BLK, HALF), 0) + i * BLK
    de_ref[...] = dot(one_hot(rows == clid_ref[0:1, :HALF]), dxc_ref[:HALF, :])

    @pl.when(jnp.max(clid_ref[0:1, HALF:]) >= 0)
    def _():
        de_ref[...] += dot(one_hot(rows == clid_ref[0:1, HALF:]), dxc_ref[HALF:, :])

    @pl.when(i == ROWS // BLK - 1)
    def _():
        total = dgp_ref[0]
        for d in range(1, TP):
            total = total + dgp_ref[d]
        dg_ref[...] = total
        keep.wait()


def finish(dxc, clid, y_in, dgp):
    vmem = pl.BlockSpec(memory_space=pltpu.VMEM)
    return pl.pallas_call(
        finish_kernel,
        grid=(ROWS // BLK,),
        out_shape=(
            jax.ShapeDtypeStruct((ROWS, HID), F32),
            jax.ShapeDtypeStruct((TOK, HID), BF16),
            jax.ShapeDtypeStruct((1, HID), F32),
        ),
        in_specs=[vmem] * 4,
        out_specs=(pl.BlockSpec((BLK, HID), lambda i: (i, 0)), pl.BlockSpec(memory_space=pltpu.HBM), vmem),
        scratch_shapes=[pltpu.SemaphoreType.DMA],
        name='finish',
    )(dxc, clid, y_in, dgp)


def swap_kernel(src_ref, dst_ref, local_sem, send_sem, recv_sem):
    me = lax.axis_index('tp')
    barrier = pltpu.get_barrier_semaphore()

    def greet(i, carry):
        pl.semaphore_signal(barrier, inc=1, device_id={'tp': (me + i) % TP}, device_id_type=MESH)
        return carry

    lax.fori_loop(1, TP, greet, 0)
    pl.semaphore_wait(barrier, TP - 1)

    def copy(i):
        peer = (me + i) % TP
        return pltpu.make_async_remote_copy(
            src_ref=src_ref.at[peer], dst_ref=dst_ref.at[me], send_sem=send_sem.at[i], recv_sem=recv_sem.at[me],
            device_id={'tp': peer}, device_id_type=MESH)

    def start(i, carry):
        copy(i).start()
        return carry

    lax.fori_loop(1, TP, start, 0)
    keep = pltpu.make_async_copy(src_ref.at[me], dst_ref.at[me], local_sem)
    keep.start()

    def wait(i, carry):
        peer = (me + i) % TP
        pltpu.make_async_remote_copy(
            src_ref=src_ref.at[peer], dst_ref=dst_ref.at[peer], send_sem=send_sem.at[i], recv_sem=recv_sem.at[peer],
            device_id={'tp': peer}, device_id_type=MESH).wait()
        return carry

    lax.fori_loop(1, TP, wait, 0)
    keep.wait()


def swap(blocks, cid):
    return pl.pallas_call(
        swap_kernel,
        out_shape=jax.ShapeDtypeStruct(blocks.shape, blocks.dtype),
        in_specs=[pl.BlockSpec(memory_space=pl.ANY)],
        out_specs=pl.BlockSpec(memory_space=pl.ANY),
        scratch_shapes=[pltpu.SemaphoreType.DMA, pltpu.SemaphoreType.DMA((TP,)), pltpu.SemaphoreType.DMA((TP,))],
        compiler_params=pltpu.CompilerParams(collective_id=cid, has_side_effects=True),
        name='swap',
    )(blocks)


def general(ids, table, gain, grad):
    local = ids.reshape(-1) - lax.axis_index('tp') * ROWS
    mine = (local >= 0) & (local < ROWS)
    looked = jnp.take(table, jnp.where(mine, local, 0), axis=0)
    parts = swap(jnp.where(mine[:, None], looked, jnp.zeros((), BF16)).reshape(TP, TOK, HID), 1)
    h = jnp.sum(parts.astype(F32), axis=0)
    inv = lax.rsqrt(jnp.mean(h * h, axis=-1, keepdims=True) + RMS_EPS)
    xh = h * inv
    y = xh.astype(BF16) * gain
    gr = grad.astype(F32)
    part = jnp.sum(gr * xh, axis=0)
    u = gr * gain.astype(F32)
    dx = (inv * (u - xh * jnp.mean(u * xh, axis=-1, keepdims=True))).astype(BF16)
    dx_all = swap(jnp.broadcast_to(dx[None], (TP, TOK, HID)), 2).reshape(SEQ, HID)
    dg = jnp.sum(swap(jnp.broadcast_to(part.reshape(1, TOK // 8, 128), (TP, TOK // 8, 128)), 3), axis=0).reshape(1, HID)
    de = jax.ops.segment_sum(dx_all.astype(F32), jnp.where(mine, local, ROWS), num_segments=ROWS)
    return de, y, dg


def device_step(token_ids, table, gain, grad):
    ids = token_ids.reshape(TP, TOK)
    gain = gain.reshape(1, HID)
    grad = grad.reshape(TOK, HID)
    dxc, clid, y_in, dgp, flag = exchange(ids, table, gain, grad)
    de, y, dg = lax.cond(
        flag[0] > 0,
        lambda: general(ids, table, gain, grad),
        lambda: finish(dxc, clid, y_in, dgp),
    )
    return y.reshape(1, TOK, HID), de, dg.reshape(HID)


def solution(mesh):
    return jax.shard_map(
        device_step, mesh=mesh,
        in_specs=(P('dp', None), P('tp', None), P(None), P('dp', 'tp', None)),
        out_specs=(P('dp', 'tp', None), P(('dp', 'tp'), None), P('dp')), check_vma=False)
```

```python
import functools

import jax
import jax.numpy as jnp
from jax import lax
from jax.experimental import pallas as pl
from jax.experimental.pallas import tpu as pltpu
from jax.sharding import PartitionSpec as P

RMS_EPS = 1e-5
TP = 16
ROWS = 3072
HID = 2048
SEQ = 2048
TOK = 128
XC = 32
DC = 56
DW = 40
NC = 512
CHUNKS = 6
MESH = pl.DeviceIdType.MESH
F32 = jnp.float32
BF16 = jnp.bfloat16
I32 = jnp.int32


def dot(a, b):
    return lax.dot_general(a, b, (((1,), (0,)), ((), ())), preferred_element_type=F32)


def one_hot(mask):
    return jnp.where(mask, 1.0, 0.0).astype(BF16)


def owner_of(ids):
    return ((ids >> 10) * 171) >> 9


def columns(rows):
    pad = jnp.zeros((128 - rows.shape[0], 128), rows.dtype)
    return jnp.concatenate([rows, pad], axis=0).T


def exchange_kernel(
    ids_ref, table_ref, gain_ref, grad_ref,
    dxc_ref, clid_ref, y_ref, dgp_ref, flag_ref,
    tbl, tbl_sem, xs, xrecv, ds, zbuf, drecv, dxs, dgs,
    xz_send, xf_send, x_sem, dz_send, z_sem, df_send, d_sem, g_send, g_sem,
):
    me = lax.axis_index('tp')
    z = me // 4
    lane = me % 4
    y = lane // 2
    c = lane % 2
    sib = z * 4 + y * 2 + (1 - c)
    ymate = z * 4 + (1 - y) * 2 + c
    zs = [z, z + 1 - 2 * (z % 2), z + 2 - 4 * (z // 2), 3 - z]

    barrier = pltpu.get_barrier_semaphore()

    def greet(i, carry):
        pl.semaphore_signal(barrier, inc=1, device_id={'tp': (me + i) % TP}, device_id_type=MESH)
        return carry

    lax.fori_loop(1, TP, greet, 0)

    part = ROWS // CHUNKS
    loads = [
        pltpu.make_async_copy(table_ref.at[pl.ds(i * part, part)], tbl.at[pl.ds(i * part, part)], tbl_sem.at[i])
        for i in range(CHUNKS)
    ]
    for load in loads:
        load.start()

    sends = []

    def send(src, dst, ssem, rsem, dev):
        cp = pltpu.make_async_remote_copy(
            src_ref=src, dst_ref=dst, send_sem=ssem, recv_sem=rsem, device_id={'tp': dev}, device_id_type=MESH)
        cp.start()
        sends.append(cp)

    def arrived(ref, sem):
        pltpu.make_async_remote_copy(
            src_ref=ref, dst_ref=ref, send_sem=xz_send.at[0], recv_sem=sem,
            device_id={'tp': sib}, device_id_type=MESH).wait_recv()

    ids = ids_ref[...]
    own = owner_of(ids)
    row_iota = lax.broadcasted_iota(I32, (TP, 128), 0)
    sub = lax.broadcasted_iota(I32, (128, 128), 0)
    lan = lax.broadcasted_iota(I32, (128, 128), 1)
    before = sub < lan

    def my_row(rows):
        return jnp.sum(jnp.where(row_iota == me, rows, 0), axis=0, keepdims=True)

    my_own = my_row(own)
    my_own_c = columns(jnp.broadcast_to(my_own, (8, 128)))[:, 0:1]
    my_chip = my_own >> 1
    same = ((my_own_c >> 1) == my_chip) & before
    my_rank = jnp.sum(jnp.where(same, 1, 0), axis=0, keepdims=True)
    my_slot = jnp.where((my_chip & 1) == 0, my_rank, DC - 1 - my_rank)
    my_zown = my_own >> 2
    dslot_iota = lax.broadcasted_iota(I32, (DC, 128), 0)

    def pack_dy(k):
        pick = (dslot_iota == my_slot) & (my_zown == zs[k])
        return dot(one_hot(pick), grad_ref[...]).astype(BF16)

    lo, hi = y * (DC - DW), (1 - y) * (DC - DW)

    def forward_z(k):
        src = zs[k] * 4 + lane
        if k:
            arrived(zbuf.at[k], z_sem.at[k])
        send(zbuf.at[k, pl.ds(pl.multiple_of(hi, 8), DW)], drecv.at[src], df_send.at[3 * k], d_sem.at[src], ymate)
        send(zbuf.at[k, pl.ds(pl.multiple_of(lo, 8), DW)], drecv.at[src], df_send.at[3 * k + 1], d_sem.at[src], sib)

    def forward_zmate(k):
        src = zs[k] * 4 + (1 - y) * 2 + c
        arrived(drecv.at[src], d_sem.at[src])
        send(drecv.at[src], drecv.at[src], df_send.at[3 * k + 2], d_sem.at[src], sib)

    def collect_dy(k):
        for j in range(2):
            src = zs[k] * 4 + ((1 - y) * 2 if j else y * 2) + (1 - c)
            arrived(drecv.at[src], d_sem.at[src])

    for k in (1, 2, 3):
        ds[k - 1] = pack_dy(k)
    zbuf[0] = pack_dy(0)
    pl.semaphore_wait(barrier, TP - 1)
    for k in (1, 2, 3):
        send(ds.at[k - 1], zbuf.at[k], dz_send.at[k - 1], z_sem.at[k], zs[k] * 4 + lane)
    forward_z(0)

    idc = columns(ids)
    dup_rows = []
    for s in range(4):
        for b in range(4):
            acc = jnp.zeros((128, 128), I32)
            row = ids[4 * s + b:4 * s + b + 1, :]
            for a in range(b + 1):
                same = idc[:, 4 * s + a:4 * s + a + 1] == row
                if a == b:
                    same = same & before
                acc = acc | jnp.where(same, 1, 0)
            dup_rows.append(jnp.max(acc, axis=0, keepdims=True))
    first = jnp.concatenate(dup_rows, axis=0) == 0
    key = jnp.where(first, own, -1)
    keyc = columns(key)
    rank_rows = []
    for s in range(4):
        for b in range(4):
            acc = jnp.zeros((128, 128), I32)
            row = own[4 * s + b:4 * s + b + 1, :]
            for a in range(b + 1):
                same = keyc[:, 4 * s + a:4 * s + a + 1] == row
                if a == b:
                    same = same & before
                acc = acc + jnp.where(same, 1, 0)
            rank_rows.append(jnp.sum(acc, axis=0, keepdims=True))
    rank = jnp.concatenate(rank_rows, axis=0)

    local = ids - me * ROWS
    mine = own == me
    xslot = jnp.where(first & mine, rank, -1)
    slot_iota = lax.broadcasted_iota(I32, (XC, 128), 0)
    lids = []
    for s in range(4):
        acc = jnp.zeros((XC, 128), I32)
        for a in range(4):
            d = 4 * s + a
            acc = acc + jnp.where(slot_iota == xslot[d:d + 1, :], local[d:d + 1, :] + 1, 0)
        lids.append(jnp.sum(acc, axis=1, keepdims=True) - 1)
    lid = jnp.concatenate(lids, axis=0)

    packed = jnp.zeros((4 * XC, HID), F32)
    chunk_iota = lax.broadcasted_iota(I32, (4 * XC, part), 1)
    for i in range(CHUNKS):
        loads[i].wait()
        packed = packed + dot(one_hot(chunk_iota + i * part == lid), tbl[pl.ds(i * part, part), :])
    packed = packed.astype(BF16)
    for s in range(4):
        xs[s] = packed[s * XC:(s + 1) * XC, :]
    xrecv[me] = xs[z]

    def forward_x(k):
        src = zs[k] * 4 + lane
        if k:
            arrived(xrecv.at[src], x_sem.at[src])
        send(xrecv.at[src], xrecv.at[src], xf_send.at[3 * k], x_sem.at[src], ymate)
        send(xrecv.at[src], xrecv.at[src], xf_send.at[3 * k + 1], x_sem.at[src], sib)

    def forward_xmate(k):
        src = zs[k] * 4 + (1 - y) * 2 + c
        arrived(xrecv.at[src], x_sem.at[src])
        send(xrecv.at[src], xrecv.at[src], xf_send.at[3 * k + 2], x_sem.at[src], sib)

    def collect_x(k):
        for j in range(2):
            src = zs[k] * 4 + ((1 - y) * 2 if j else y * 2) + (1 - c)
            arrived(xrecv.at[src], x_sem.at[src])

    for k in (1, 2, 3):
        send(xs.at[zs[k]], xrecv.at[me], xz_send.at[k - 1], x_sem.at[me], zs[k] * 4 + lane)
    forward_x(0)
    forward_z(1)
    forward_zmate(0)

    over = jnp.max(jnp.where(first & (rank >= XC), 1, 0))

    def slab(rows):
        out = jnp.zeros((4, 128), I32)
        for s in range(4):
            out = out + jnp.where(z == s, rows[4 * s:4 * s + 4, :], 0)
        return out

    tslot = slab(jnp.where(first & (rank < XC), own * XC + rank, -1))
    mine_c = columns(jnp.concatenate([tslot, slab(ids), jnp.broadcast_to(my_row(ids), (8, 128))], axis=0))
    my_ids_c = mine_c[:, 8:9]
    spread = []
    for q in range(4):
        acc = jnp.zeros((128, 128), I32)
        for a in range(4):
            acc = acc + jnp.where(mine_c[:, a:a + 1] == lan + q * 128, mine_c[:, 4 + a:5 + a] + 1, 0)
        spread.append(one_hot(my_ids_c == jnp.sum(acc, axis=0, keepdims=True) - 1))
    spread = jnp.concatenate(spread, axis=1)

    chip_c = ((idc >> 10) * 171) >> 10
    chip = own >> 1
    drank_rows = []
    for d in range(TP):
        same = (chip_c[:, d:d + 1] == chip[d:d + 1, :]) & before
        drank_rows.append(jnp.sum(jnp.where(same, 1, 0), axis=0, keepdims=True))
    drank = jnp.concatenate(drank_rows, axis=0)
    over = jnp.maximum(over, jnp.max(jnp.where(drank >= DW, 1, 0)))
    for s in range(4):
        in_slab = jnp.sum(jnp.where((own >> 2) == s, 1.0, 0.0), axis=1, keepdims=True)
        over = jnp.maximum(over, jnp.max(jnp.where(in_slab > DC, 1, 0)))
    for o in range(TP):
        over = jnp.maximum(over, jnp.where(jnp.sum(jnp.where(own == o, 1.0, 0.0)) > NC, 1, 0))
    flag_ref[0] = over
    forward_xmate(0)

    dslot = jnp.where(mine & (drank < DW), jnp.where(y == 0, drank, DW - 1 - drank), -1)
    dslot_c = columns(dslot)
    lrows = []
    for p in range(TP * DW // 128):
        acc = jnp.zeros((128, 128), I32)
        for d in range(TP):
            if d * DW < (p + 1) * 128 and (d + 1) * DW > p * 128:
                sc = dslot_c[:, d:d + 1]
                acc = acc + jnp.where((sc >= 0) & (sc + (d * DW - p * 128) == lan), idc[:, d:d + 1] - me * ROWS + 1, 0)
        lrows.append(jnp.sum(acc, axis=0, keepdims=True))
    lid1 = jnp.concatenate(lrows + [jnp.zeros((8 - len(lrows), 128), I32)], axis=0)
    has = lid1 > 0
    has_f = jnp.where(has, 1.0, 0.0)
    inrow = dot(has_f.astype(BF16), one_hot(before))
    total = jnp.sum(has_f, axis=1, keepdims=True)
    crank_rows = []
    base = jnp.zeros((1, 1), F32)
    for p in range(8):
        crank_rows.append(inrow[p:p + 1, :] + base)
        base = base + total[p:p + 1, :]
    crank = jnp.where(has, jnp.concatenate(crank_rows, axis=0).astype(I32), -1)
    n_iota = lax.broadcasted_iota(I32, (NC, 128), 0)
    compact = jnp.concatenate([one_hot(n_iota == crank[p:p + 1, :]) for p in range(len(lrows))], axis=1)
    lrow = jnp.concatenate([lid1[p:p + 1, :] for p in range(len(lrows))], axis=1)
    halves = jnp.concatenate([lrow >> 6, lrow & 63, jnp.zeros((6, TP * DW), I32)], axis=0).astype(F32).astype(BF16)
    cl = lax.dot_general(halves, compact, (((1,), (1,)), ((), ())), preferred_element_type=F32)
    clid_ref[...] = jnp.broadcast_to((cl[0:1, :] * 64.0 + cl[1:2, :]).astype(I32) - 1, (8, NC))

    gain = gain_ref[...].reshape(1, HID)
    gain_f = gain.astype(F32)
    xlid = jnp.broadcast_to(lid, (4 * XC, 128)).T[0:1, :]
    w_iota = lax.broadcasted_iota(I32, (DW, 128), 0)
    x_group = lax.broadcasted_iota(I32, (1, 4 * XC), 1) // XC

    steps = [(r0, min(16, DW - r0)) for r0 in range(0, DW, 16)]

    def dx_rows(zk, dy_of, gain_sum):
        pick_row = jnp.where(x_group == zk, xlid, -2)
        for block, at in dy_of:
            slot_row = jnp.sum(jnp.where(row_iota == at, dslot, 0), axis=0, keepdims=True)
            local_row = jnp.sum(jnp.where(row_iota == at, local, 0), axis=0, keepdims=True)
            dlid = jnp.sum(jnp.where(w_iota == slot_row, local_row + 1, 0), axis=1, keepdims=True) - 1
            h_all = dot(one_hot(dlid == pick_row), jnp.concatenate([xs[s] for s in range(4)], axis=0))
            for r0, n in steps:
                h = h_all[r0:r0 + n, :]
                inv = lax.rsqrt(jnp.mean(h * h, axis=-1, keepdims=True) + RMS_EPS)
                xh = h * inv
                gr = block(r0, n).astype(F32)
                gain_sum = gain_sum + jnp.sum(gr * xh, axis=0, keepdims=True)
                u = gr * gain_f
                dx = inv * (u - xh * jnp.mean(u * xh, axis=-1, keepdims=True))
                dxs[at, pl.ds(r0, n), :] = dx.astype(BF16)
        return gain_sum

    def process(k, gain_sum):
        collect_dy(k)
        zk = zs[k]
        out = [(lambda r0, n: zbuf[k, pl.ds(pl.multiple_of(lo + r0, 8), n), :], zk * 4 + lane)]
        for off in ((1 - y) * 2 + c, y * 2 + (1 - c), (1 - y) * 2 + (1 - c)):
            at = zk * 4 + off
            out.append((lambda r0, n, at=at: drecv[at, pl.ds(r0, n), :], at))
        return dx_rows(zk, out, gain_sum)

    forward_z(2)
    forward_zmate(1)
    gain_sum = process(0, jnp.zeros((1, HID), F32))
    forward_z(3)
    forward_zmate(2)
    gain_sum = process(1, gain_sum)
    forward_x(1)
    forward_zmate(3)
    gain_sum = process(2, gain_sum)
    forward_x(2)
    forward_xmate(1)
    gain_sum = process(3, gain_sum)
    dgs[...] = gain_sum
    dgp_ref[me] = gain_sum
    for i in range(1, TP):
        send(dgs, dgp_ref.at[me], g_send.at[i - 1], g_sem.at[me], (me + i) % TP)
    forward_x(3)
    forward_xmate(2)
    dxc_ref[...] = dot(compact, jnp.concatenate([dxs[d] for d in range(TP)], axis=0)).astype(BF16)
    forward_xmate(3)
    for k in range(4):
        collect_x(k)
    h_all = dot(spread, jnp.concatenate([xrecv[d] for d in range(TP)], axis=0))
    for r0 in range(0, TOK, 16):
        h = h_all[r0:r0 + 16, :]
        xh = h * lax.rsqrt(jnp.mean(h * h, axis=-1, keepdims=True) + RMS_EPS)
        y_ref[pl.ds(r0, 16), :] = xh.astype(BF16) * gain
    for i in range(1, TP):
        src = (me + i) % TP
        arrived(dgp_ref.at[src], g_sem.at[src])
    for cp in sends:
        cp.wait_send()


def exchange(ids, table, gain, grad):
    vmem = pl.BlockSpec(memory_space=pltpu.VMEM)
    dma = pltpu.SemaphoreType.DMA
    return pl.pallas_call(
        exchange_kernel,
        out_shape=(
            pltpu.VMEM((NC, HID), BF16),
            pltpu.VMEM((8, NC), I32),
            pltpu.VMEM((TOK, HID), BF16),
            pltpu.VMEM((TP, 1, HID), F32),
            jax.ShapeDtypeStruct((1,), I32),
        ),
        in_specs=[vmem, pl.BlockSpec(memory_space=pltpu.HBM), vmem, vmem],
        out_specs=(vmem, vmem, vmem, vmem, pl.BlockSpec(memory_space=pltpu.SMEM)),
        scratch_shapes=[
            pltpu.VMEM((ROWS, HID), BF16),
            dma((CHUNKS,)),
            pltpu.VMEM((4, XC, HID), BF16),
            pltpu.VMEM((TP, XC, HID), BF16),
            pltpu.VMEM((3, DC, HID), BF16),
            pltpu.VMEM((4, DC, HID), BF16),
            pltpu.VMEM((TP, DW, HID), BF16),
            pltpu.VMEM((TP, DW, HID), BF16),
            pltpu.VMEM((1, HID), F32),
            dma((3,)), dma((12,)), dma((TP,)), dma((3,)), dma((4,)), dma((12,)), dma((TP,)), dma((TP - 1,)), dma((TP,)),
        ],
        compiler_params=pltpu.CompilerParams(collective_id=0, has_side_effects=True, vmem_limit_bytes=44 << 20),
        name='exchange',
    )(ids, table, gain, grad)


BLK = 128
SLOTS = 8
HALF = NC // 2


def finish_kernel(dxc_ref, clid_ref, y_in_ref, dgp_ref, de_ref, y_ref, dg_ref, buf, dg_s, sem, buf_sem):
    steps = ROWS // BLK
    keep_y = pltpu.make_async_copy(y_in_ref, y_ref, sem.at[0])
    keep_y.start()
    more = jnp.max(clid_ref[0:1, HALF:]) >= 0

    def out(i):
        slot = lax.rem(i, SLOTS)
        return pltpu.make_async_copy(buf.at[slot], de_ref.at[pl.ds(pl.multiple_of(i * BLK, BLK), BLK)], buf_sem.at[slot])

    def step(i, carry):
        @pl.when(i >= SLOTS)
        def _():
            out(i - SLOTS).wait()

        slot = lax.rem(i, SLOTS)
        rows = lax.broadcasted_iota(I32, (BLK, HALF), 0) + i * BLK
        buf[slot] = dot(one_hot(rows == clid_ref[0:1, :HALF]), dxc_ref[:HALF, :])

        @pl.when(more)
        def _():
            buf[slot] += dot(one_hot(rows == clid_ref[0:1, HALF:]), dxc_ref[HALF:, :])

        out(i).start()
        return carry

    lax.fori_loop(0, steps, step, 0)
    total = dgp_ref[0]
    for d in range(1, TP):
        total = total + dgp_ref[d]
    dg_s[...] = total
    keep_dg = pltpu.make_async_copy(dg_s, dg_ref, sem.at[1])
    keep_dg.start()

    def drain(i, carry):
        out(i).wait()
        return carry

    lax.fori_loop(steps - SLOTS, steps, drain, 0)
    keep_y.wait()
    keep_dg.wait()


def finish(dxc, clid, y_in, dgp):
    vmem = pl.BlockSpec(memory_space=pltpu.VMEM)
    hbm = pl.BlockSpec(memory_space=pltpu.HBM)
    return pl.pallas_call(
        finish_kernel,
        out_shape=(
            pltpu.HBM((ROWS, HID), F32),
            pltpu.HBM((TOK, HID), BF16),
            pltpu.HBM((1, HID), F32),
        ),
        in_specs=[vmem] * 4,
        out_specs=(hbm, hbm, hbm),
        scratch_shapes=[
            pltpu.VMEM((SLOTS, BLK, HID), F32),
            pltpu.VMEM((1, HID), F32),
            pltpu.SemaphoreType.DMA((2,)),
            pltpu.SemaphoreType.DMA((SLOTS,)),
        ],
        compiler_params=pltpu.CompilerParams(vmem_limit_bytes=24 << 20),
        name='finish',
    )(dxc, clid, y_in, dgp)


def swap_kernel(src_ref, dst_ref, local_sem, send_sem, recv_sem):
    me = lax.axis_index('tp')
    barrier = pltpu.get_barrier_semaphore()

    def greet(i, carry):
        pl.semaphore_signal(barrier, inc=1, device_id={'tp': (me + i) % TP}, device_id_type=MESH)
        return carry

    lax.fori_loop(1, TP, greet, 0)
    pl.semaphore_wait(barrier, TP - 1)

    def copy(i):
        peer = (me + i) % TP
        return pltpu.make_async_remote_copy(
            src_ref=src_ref.at[peer], dst_ref=dst_ref.at[me], send_sem=send_sem.at[i], recv_sem=recv_sem.at[me],
            device_id={'tp': peer}, device_id_type=MESH)

    def start(i, carry):
        copy(i).start()
        return carry

    lax.fori_loop(1, TP, start, 0)
    keep = pltpu.make_async_copy(src_ref.at[me], dst_ref.at[me], local_sem)
    keep.start()

    def wait(i, carry):
        peer = (me + i) % TP
        pltpu.make_async_remote_copy(
            src_ref=src_ref.at[peer], dst_ref=dst_ref.at[peer], send_sem=send_sem.at[i], recv_sem=recv_sem.at[peer],
            device_id={'tp': peer}, device_id_type=MESH).wait()
        return carry

    lax.fori_loop(1, TP, wait, 0)
    keep.wait()


def swap(blocks, cid):
    return pl.pallas_call(
        swap_kernel,
        out_shape=jax.ShapeDtypeStruct(blocks.shape, blocks.dtype),
        in_specs=[pl.BlockSpec(memory_space=pl.ANY)],
        out_specs=pl.BlockSpec(memory_space=pl.ANY),
        scratch_shapes=[pltpu.SemaphoreType.DMA, pltpu.SemaphoreType.DMA((TP,)), pltpu.SemaphoreType.DMA((TP,))],
        compiler_params=pltpu.CompilerParams(collective_id=cid, has_side_effects=True),
        name='swap',
    )(blocks)


def general(ids, table, gain, grad):
    local = ids.reshape(-1) - lax.axis_index('tp') * ROWS
    mine = (local >= 0) & (local < ROWS)
    looked = jnp.take(table, jnp.where(mine, local, 0), axis=0)
    parts = swap(jnp.where(mine[:, None], looked, jnp.zeros((), BF16)).reshape(TP, TOK, HID), 1)
    h = jnp.sum(parts.astype(F32), axis=0)
    inv = lax.rsqrt(jnp.mean(h * h, axis=-1, keepdims=True) + RMS_EPS)
    xh = h * inv
    y = xh.astype(BF16) * gain
    gr = grad.astype(F32)
    part = jnp.sum(gr * xh, axis=0)
    u = gr * gain.astype(F32)
    dx = (inv * (u - xh * jnp.mean(u * xh, axis=-1, keepdims=True))).astype(BF16)
    dx_all = swap(jnp.broadcast_to(dx[None], (TP, TOK, HID)), 2).reshape(SEQ, HID)
    dg = jnp.sum(swap(jnp.broadcast_to(part.reshape(1, TOK // 8, 128), (TP, TOK // 8, 128)), 3), axis=0).reshape(1, HID)
    de = jax.ops.segment_sum(dx_all.astype(F32), jnp.where(mine, local, ROWS), num_segments=ROWS)
    return de, y, dg


def device_step(token_ids, table, gain, grad):
    ids = token_ids.reshape(TP, TOK)
    grad = grad.reshape(TOK, HID)
    dxc, clid, y_in, dgp, flag = exchange(ids, table, gain, grad)
    de, y, dg = lax.cond(
        flag[0] > 0,
        lambda: general(ids, table, gain, grad),
        lambda: finish(dxc, clid, y_in, dgp),
    )
    return y.reshape(1, TOK, HID), de, dg.reshape(HID)


def solution(mesh):
    return jax.shard_map(
        device_step, mesh=mesh,
        in_specs=(P('dp', None), P('tp', None), P(None), P('dp', 'tp', None)),
        out_specs=(P('dp', 'tp', None), P(('dp', 'tp'), None), P('dp')), check_vma=False)
```

```python
import functools

import jax
import jax.numpy as jnp
from jax import lax
from jax.experimental import pallas as pl
from jax.experimental.pallas import tpu as pltpu
from jax.sharding import PartitionSpec as P

RMS_EPS = 1e-5
TP = 16
ROWS = 3072
HID = 2048
SEQ = 2048
TOK = 128
XC = 32
DC = 56
DW = 40
NC = 384
CHUNKS = 6
MESH = pl.DeviceIdType.MESH
F32 = jnp.float32
BF16 = jnp.bfloat16
I32 = jnp.int32


def dot(a, b):
    return lax.dot_general(a, b, (((1,), (0,)), ((), ())), preferred_element_type=F32)


def one_hot(mask):
    return jnp.where(mask, 1.0, 0.0).astype(BF16)


def owner_of(ids):
    return ((ids >> 10) * 171) >> 9


def columns(rows):
    pad = jnp.zeros((128 - rows.shape[0], 128), rows.dtype)
    return jnp.concatenate([rows, pad], axis=0).T


def exchange_kernel(
    ids_hbm, table_ref, gain_hbm, grad_hbm,
    dxc_ref, clid_ref, y_ref, dgp_ref, flag_ref,
    ids_ref, gain_ref, grad_ref, in_sem, tbl, tbl_sem, xs, xrecv, ds, zbuf, drecv, dxs, dgs,
    xz_send, xf_send, x_sem, dz_send, z_sem, df_send, d_sem, g_send, g_sem,
):
    me = lax.axis_index('tp')
    z = me // 4
    lane = me % 4
    y = lane // 2
    c = lane % 2
    sib = z * 4 + y * 2 + (1 - c)
    ymate = z * 4 + (1 - y) * 2 + c
    zs = [z, z + 1 - 2 * (z % 2), z + 2 - 4 * (z // 2), 3 - z]

    barrier = pltpu.get_barrier_semaphore()

    def greet(i, carry):
        pl.semaphore_signal(barrier, inc=1, device_id={'tp': (me + i) % TP}, device_id_type=MESH)
        return carry

    lax.fori_loop(1, TP, greet, 0)

    first_loads = [
        pltpu.make_async_copy(src, dst, in_sem.at[i])
        for i, (src, dst) in enumerate(((ids_hbm, ids_ref), (grad_hbm, grad_ref), (gain_hbm, gain_ref)))
    ]
    for load in first_loads:
        load.start()
    part = ROWS // CHUNKS
    loads = [
        pltpu.make_async_copy(table_ref.at[pl.ds(i * part, part)], tbl.at[pl.ds(i * part, part)], tbl_sem.at[i])
        for i in range(CHUNKS)
    ]
    for load in loads:
        load.start()

    sends = []

    def send(src, dst, ssem, rsem, dev):
        cp = pltpu.make_async_remote_copy(
            src_ref=src, dst_ref=dst, send_sem=ssem, recv_sem=rsem, device_id={'tp': dev}, device_id_type=MESH)
        cp.start()
        sends.append(cp)

    def arrived(ref, sem):
        pltpu.make_async_remote_copy(
            src_ref=ref, dst_ref=ref, send_sem=xz_send.at[0], recv_sem=sem,
            device_id={'tp': sib}, device_id_type=MESH).wait_recv()

    first_loads[0].wait()
    ids = ids_ref[...]
    own = owner_of(ids)
    row_iota = lax.broadcasted_iota(I32, (TP, 128), 0)
    sub = lax.broadcasted_iota(I32, (128, 128), 0)
    lan = lax.broadcasted_iota(I32, (128, 128), 1)
    before = sub < lan

    def my_row(rows):
        return jnp.sum(jnp.where(row_iota == me, rows, 0), axis=0, keepdims=True)

    my_own = my_row(own)
    my_own_c = columns(jnp.broadcast_to(my_own, (8, 128)))[:, 0:1]
    my_chip = my_own >> 1
    same = ((my_own_c >> 1) == my_chip) & before
    my_rank = jnp.sum(jnp.where(same, 1, 0), axis=0, keepdims=True)
    my_slot = jnp.where((my_chip & 1) == 0, my_rank, DC - 1 - my_rank)
    my_zown = my_own >> 2
    dslot_iota = lax.broadcasted_iota(I32, (DC, 128), 0)

    def pack_dy(k):
        pick = (dslot_iota == my_slot) & (my_zown == zs[k])
        return dot(one_hot(pick), grad_ref[...]).astype(BF16)

    lo, hi = y * (DC - DW), (1 - y) * (DC - DW)

    def forward_z(k):
        src = zs[k] * 4 + lane
        if k:
            arrived(zbuf.at[k], z_sem.at[k])
        send(zbuf.at[k, pl.ds(pl.multiple_of(hi, 8), DW)], drecv.at[src], df_send.at[3 * k], d_sem.at[src], ymate)
        send(zbuf.at[k, pl.ds(pl.multiple_of(lo, 8), DW)], drecv.at[src], df_send.at[3 * k + 1], d_sem.at[src], sib)

    def forward_zmate(k):
        src = zs[k] * 4 + (1 - y) * 2 + c
        arrived(drecv.at[src], d_sem.at[src])
        send(drecv.at[src], drecv.at[src], df_send.at[3 * k + 2], d_sem.at[src], sib)

    def collect_dy(k):
        for j in range(2):
            src = zs[k] * 4 + ((1 - y) * 2 if j else y * 2) + (1 - c)
            arrived(drecv.at[src], d_sem.at[src])

    def send_dy(k):
        send(ds.at[k - 1], zbuf.at[k], dz_send.at[k - 1], z_sem.at[k], zs[k] * 4 + lane)

    first_loads[1].wait()
    first_loads[2].wait()
    ds[0] = pack_dy(1)
    pl.semaphore_wait(barrier, TP - 1)
    send_dy(1)
    zbuf[0] = pack_dy(0)
    forward_z(0)
    ds[1] = pack_dy(2)
    send_dy(2)
    ds[2] = pack_dy(3)

    idc = columns(ids)
    dup_rows = []
    for s in range(4):
        for b in range(4):
            acc = jnp.zeros((128, 128), I32)
            row = ids[4 * s + b:4 * s + b + 1, :]
            for a in range(b + 1):
                same = idc[:, 4 * s + a:4 * s + a + 1] == row
                if a == b:
                    same = same & before
                acc = acc | jnp.where(same, 1, 0)
            dup_rows.append(jnp.max(acc, axis=0, keepdims=True))
    first = jnp.concatenate(dup_rows, axis=0) == 0
    key = jnp.where(first, own, -1)
    keyc = columns(key)
    rank_rows = []
    for s in range(4):
        for b in range(4):
            acc = jnp.zeros((128, 128), I32)
            row = own[4 * s + b:4 * s + b + 1, :]
            for a in range(b + 1):
                same = keyc[:, 4 * s + a:4 * s + a + 1] == row
                if a == b:
                    same = same & before
                acc = acc + jnp.where(same, 1, 0)
            rank_rows.append(jnp.sum(acc, axis=0, keepdims=True))
    rank = jnp.concatenate(rank_rows, axis=0)

    local = ids - me * ROWS
    mine = own == me
    xslot = jnp.where(first & mine, rank, -1)
    slot_iota = lax.broadcasted_iota(I32, (XC, 128), 0)
    lids = []
    for s in range(4):
        acc = jnp.zeros((XC, 128), I32)
        for a in range(4):
            d = 4 * s + a
            acc = acc + jnp.where(slot_iota == xslot[d:d + 1, :], local[d:d + 1, :] + 1, 0)
        lids.append(jnp.sum(acc, axis=1, keepdims=True) - 1)
    lid = jnp.concatenate(lids, axis=0)

    packed = jnp.zeros((4 * XC, HID), F32)
    chunk_iota = lax.broadcasted_iota(I32, (4 * XC, part), 1)
    for i in range(CHUNKS):
        loads[i].wait()
        packed = packed + dot(one_hot(chunk_iota + i * part == lid), tbl[pl.ds(i * part, part), :])
    packed = packed.astype(BF16)
    for s in range(4):
        xs[s] = packed[s * XC:(s + 1) * XC, :]
    xrecv[me] = xs[z]

    def forward_x(k):
        src = zs[k] * 4 + lane
        if k:
            arrived(xrecv.at[src], x_sem.at[src])
        send(xrecv.at[src], xrecv.at[src], xf_send.at[3 * k], x_sem.at[src], ymate)
        send(xrecv.at[src], xrecv.at[src], xf_send.at[3 * k + 1], x_sem.at[src], sib)

    def forward_xmate(k):
        src = zs[k] * 4 + (1 - y) * 2 + c
        arrived(xrecv.at[src], x_sem.at[src])
        send(xrecv.at[src], xrecv.at[src], xf_send.at[3 * k + 2], x_sem.at[src], sib)

    def collect_x(k):
        for j in range(2):
            src = zs[k] * 4 + ((1 - y) * 2 if j else y * 2) + (1 - c)
            arrived(xrecv.at[src], x_sem.at[src])

    for k in (1, 2, 3):
        send(xs.at[zs[k]], xrecv.at[me], xz_send.at[k - 1], x_sem.at[me], zs[k] * 4 + lane)
    forward_x(0)
    send_dy(3)
    forward_z(1)
    forward_zmate(0)

    over = jnp.max(jnp.where(first & (rank >= XC), 1, 0))

    def slab(rows):
        out = jnp.zeros((4, 128), I32)
        for s in range(4):
            out = out + jnp.where(z == s, rows[4 * s:4 * s + 4, :], 0)
        return out

    tslot = slab(jnp.where(first & (rank < XC), own * XC + rank, -1))
    mine_c = columns(jnp.concatenate([tslot, slab(ids), jnp.broadcast_to(my_row(ids), (8, 128))], axis=0))
    my_ids_c = mine_c[:, 8:9]
    spread = []
    for q in range(4):
        acc = jnp.zeros((128, 128), I32)
        for a in range(4):
            acc = acc + jnp.where(mine_c[:, a:a + 1] == lan + q * 128, mine_c[:, 4 + a:5 + a] + 1, 0)
        spread.append(one_hot(my_ids_c == jnp.sum(acc, axis=0, keepdims=True) - 1))
    spread = jnp.concatenate(spread, axis=1)

    chip_c = ((idc >> 10) * 171) >> 10
    chip = own >> 1
    drank_rows = []
    for d in range(TP):
        same = (chip_c[:, d:d + 1] == chip[d:d + 1, :]) & before
        drank_rows.append(jnp.sum(jnp.where(same, 1, 0), axis=0, keepdims=True))
    drank = jnp.concatenate(drank_rows, axis=0)
    over = jnp.maximum(over, jnp.max(jnp.where(drank >= DW, 1, 0)))
    for s in range(4):
        in_slab = jnp.sum(jnp.where((own >> 2) == s, 1.0, 0.0), axis=1, keepdims=True)
        over = jnp.maximum(over, jnp.max(jnp.where(in_slab > DC, 1, 0)))
    for o in range(TP):
        over = jnp.maximum(over, jnp.where(jnp.sum(jnp.where(own == o, 1.0, 0.0)) > NC, 1, 0))
    flag_ref[0] = over
    forward_xmate(0)

    def by_group(rows):
        out = []
        for k in range(4):
            part_k = jnp.zeros((4, 128), I32)
            for s in range(4):
                part_k = part_k + jnp.where(zs[k] == s, rows[4 * s:4 * s + 4, :], 0)
            out.append(part_k)
        return jnp.concatenate(out, axis=0)

    dslot = by_group(jnp.where(mine & (drank < DW), jnp.where(y == 0, drank, DW - 1 - drank), -1))
    dlocal = by_group(local)
    dslot_c = columns(jnp.concatenate([dslot, dlocal], axis=0))
    lrows = []
    for p in range(TP * DW // 128):
        acc = jnp.zeros((128, 128), I32)
        for d in range(TP):
            if d * DW < (p + 1) * 128 and (d + 1) * DW > p * 128:
                sc = dslot_c[:, d:d + 1]
                acc = acc + jnp.where((sc >= 0) & (sc + (d * DW - p * 128) == lan), dslot_c[:, TP + d:TP + d + 1] + 1, 0)
        lrows.append(jnp.sum(acc, axis=0, keepdims=True))
    lid1 = jnp.concatenate(lrows + [jnp.zeros((8 - len(lrows), 128), I32)], axis=0)
    has = lid1 > 0
    has_f = jnp.where(has, 1.0, 0.0)
    inrow = dot(has_f.astype(BF16), one_hot(before))
    total = jnp.sum(has_f, axis=1, keepdims=True)
    crank_rows = []
    base = jnp.zeros((1, 1), F32)
    for p in range(8):
        crank_rows.append(inrow[p:p + 1, :] + base)
        base = base + total[p:p + 1, :]
    crank = jnp.where(has, jnp.concatenate(crank_rows, axis=0).astype(I32), -1)
    n_iota = lax.broadcasted_iota(I32, (NC, 128), 0)
    compact = jnp.concatenate([one_hot(n_iota == crank[p:p + 1, :]) for p in range(len(lrows))], axis=1)
    lrow = jnp.concatenate([lid1[p:p + 1, :] for p in range(len(lrows))], axis=1)
    halves = jnp.concatenate([lrow >> 6, lrow & 63, jnp.zeros((6, TP * DW), I32)], axis=0).astype(F32).astype(BF16)
    cl = lax.dot_general(halves, compact, (((1,), (1,)), ((), ())), preferred_element_type=F32)
    clid_ref[...] = jnp.broadcast_to((cl[0:1, :] * 64.0 + cl[1:2, :]).astype(I32) - 1, (8, NC))

    gain = gain_ref[...].reshape(1, HID)
    gain_f = gain.astype(F32)
    xlid = jnp.broadcast_to(lid, (4 * XC, 128)).T[0:1, :]
    w_iota = lax.broadcasted_iota(I32, (DW, 128), 0)
    x_group = lax.broadcasted_iota(I32, (1, 4 * XC), 1) // XC

    steps = [(r0, min(16, DW - r0)) for r0 in range(0, DW, 16)]

    def dx_block(k, off, block):
        at = 4 * k + off
        slot_row = jnp.sum(jnp.where(row_iota == at, dslot, 0), axis=0, keepdims=True)
        local_row = jnp.sum(jnp.where(row_iota == at, dlocal, 0), axis=0, keepdims=True)
        dlid = jnp.sum(jnp.where(w_iota == slot_row, local_row + 1, 0), axis=1, keepdims=True) - 1
        pick = one_hot(dlid == jnp.where(x_group == zs[k], xlid, -2))
        h_all = dot(pick, jnp.concatenate([xs[s] for s in range(4)], axis=0))
        for r0, n in steps:
            h = h_all[r0:r0 + n, :]
            inv = lax.rsqrt(jnp.mean(h * h, axis=-1, keepdims=True) + RMS_EPS)
            xh = h * inv
            u = block(r0, n).astype(F32) * gain_f
            dx = inv * (u - xh * jnp.mean(u * xh, axis=-1, keepdims=True))
            dxs[at, pl.ds(r0, n), :] = dx.astype(BF16)

    def own_block(k):
        dx_block(k, lane, lambda r0, n: zbuf[k, pl.ds(pl.multiple_of(lo + r0, 8), n), :])

    def got_block(k, off):
        at = zs[k] * 4 + off
        dx_block(k, off, lambda r0, n: drecv[at, pl.ds(r0, n), :])

    mate_off, sib_off, far_off = (1 - y) * 2 + c, y * 2 + (1 - c), (1 - y) * 2 + (1 - c)

    def process(k):
        own_block(k)
        got_block(k, mate_off)
        collect_dy(k)
        got_block(k, sib_off)
        got_block(k, far_off)

    forward_z(2)
    forward_zmate(1)
    process(0)
    forward_x(1)
    forward_zmate(2)
    process(1)
    forward_x(2)
    forward_xmate(1)
    process(2)
    forward_x(3)
    forward_xmate(2)
    early = 12 * DW
    dxc_ref[...] = dot(compact[:, :early], jnp.concatenate([dxs[d] for d in range(12)], axis=0)).astype(BF16)
    forward_z(3)
    forward_xmate(3)
    own_block(3)
    for k in range(4):
        collect_x(k)
    h_all = dot(spread, jnp.concatenate([xrecv[d] for d in range(TP)], axis=0))
    gain_sum = jnp.zeros((1, HID), F32)
    for r0 in range(0, TOK, 16):
        h = h_all[r0:r0 + 16, :]
        xh = h * lax.rsqrt(jnp.mean(h * h, axis=-1, keepdims=True) + RMS_EPS)
        y_ref[pl.ds(r0, 16), :] = xh.astype(BF16) * gain
        gain_sum = gain_sum + jnp.sum(grad_ref[pl.ds(r0, 16), :].astype(F32) * xh, axis=0, keepdims=True)
    dgs[...] = gain_sum
    dgp_ref[me] = gain_sum
    for i in range(1, TP):
        send(dgs, dgp_ref.at[me], g_send.at[i - 1], g_sem.at[me], (me + i) % TP)
    forward_zmate(3)
    got_block(3, mate_off)
    collect_dy(3)
    got_block(3, sib_off)
    got_block(3, far_off)
    late = dot(compact[:, early:], jnp.concatenate([dxs[d] for d in range(12, TP)], axis=0))
    dxc_ref[...] += late.astype(BF16)
    for i in range(1, TP):
        src = (me + i) % TP
        arrived(dgp_ref.at[src], g_sem.at[src])
    for cp in sends:
        cp.wait_send()


def exchange(ids, table, gain, grad):
    vmem = pl.BlockSpec(memory_space=pltpu.VMEM)
    dma = pltpu.SemaphoreType.DMA
    return pl.pallas_call(
        exchange_kernel,
        out_shape=(
            pltpu.VMEM((NC, HID), BF16),
            pltpu.VMEM((8, NC), I32),
            pltpu.VMEM((TOK, HID), BF16),
            pltpu.VMEM((TP, 1, HID), F32),
            pltpu.SMEM((1,), I32),
        ),
        in_specs=[pl.BlockSpec(memory_space=pltpu.HBM)] * 4,
        out_specs=(vmem, vmem, vmem, vmem, pl.BlockSpec(memory_space=pltpu.SMEM)),
        scratch_shapes=[
            pltpu.VMEM((TP, TOK), I32),
            pltpu.VMEM((HID,), BF16),
            pltpu.VMEM((TOK, HID), BF16),
            dma((3,)),
            pltpu.VMEM((ROWS, HID), BF16),
            dma((CHUNKS,)),
            pltpu.VMEM((4, XC, HID), BF16),
            pltpu.VMEM((TP, XC, HID), BF16),
            pltpu.VMEM((3, DC, HID), BF16),
            pltpu.VMEM((4, DC, HID), BF16),
            pltpu.VMEM((TP, DW, HID), BF16),
            pltpu.VMEM((TP, DW, HID), BF16),
            pltpu.VMEM((1, HID), F32),
            dma((3,)), dma((12,)), dma((TP,)), dma((3,)), dma((4,)), dma((12,)), dma((TP,)), dma((TP - 1,)), dma((TP,)),
        ],
        compiler_params=pltpu.CompilerParams(collective_id=0, has_side_effects=True, vmem_limit_bytes=44 << 20),
        name='exchange',
    )(ids, table, gain, grad)


BLK = 128
SLOTS = 8
HALF = 256


def finish_kernel(dxc_ref, clid_ref, y_in_ref, dgp_ref, de_ref, y_ref, dg_ref, buf, dg_s, sem, buf_sem):
    steps = ROWS // BLK
    keep_y = pltpu.make_async_copy(y_in_ref, y_ref, sem.at[0])
    keep_y.start()
    more = jnp.max(clid_ref[0:1, HALF:]) >= 0

    def out(i):
        slot = lax.rem(i, SLOTS)
        return pltpu.make_async_copy(buf.at[slot], de_ref.at[pl.ds(pl.multiple_of(i * BLK, BLK), BLK)], buf_sem.at[slot])

    def step(i, carry):
        @pl.when(i >= SLOTS)
        def _():
            out(i - SLOTS).wait()

        slot = lax.rem(i, SLOTS)
        rows = lax.broadcasted_iota(I32, (BLK, HALF), 0) + i * BLK
        buf[slot] = dot(one_hot(rows == clid_ref[0:1, :HALF]), dxc_ref[:HALF, :])

        @pl.when(more)
        def _():
            buf[slot] += dot(one_hot(rows[:, :NC - HALF] == clid_ref[0:1, HALF:]), dxc_ref[HALF:, :])

        out(i).start()
        return carry

    lax.fori_loop(0, steps, step, 0)
    total = dgp_ref[0]
    for d in range(1, TP):
        total = total + dgp_ref[d]
    dg_s[...] = total
    keep_dg = pltpu.make_async_copy(dg_s, dg_ref, sem.at[1])
    keep_dg.start()

    def drain(i, carry):
        out(i).wait()
        return carry

    lax.fori_loop(steps - SLOTS, steps, drain, 0)
    keep_y.wait()
    keep_dg.wait()


def finish(dxc, clid, y_in, dgp):
    vmem = pl.BlockSpec(memory_space=pltpu.VMEM)
    hbm = pl.BlockSpec(memory_space=pltpu.HBM)
    return pl.pallas_call(
        finish_kernel,
        out_shape=(
            pltpu.HBM((ROWS, HID), F32),
            pltpu.HBM((TOK, HID), BF16),
            pltpu.HBM((1, HID), F32),
        ),
        in_specs=[vmem] * 4,
        out_specs=(hbm, hbm, hbm),
        scratch_shapes=[
            pltpu.VMEM((SLOTS, BLK, HID), F32),
            pltpu.VMEM((1, HID), F32),
            pltpu.SemaphoreType.DMA((2,)),
            pltpu.SemaphoreType.DMA((SLOTS,)),
        ],
        compiler_params=pltpu.CompilerParams(vmem_limit_bytes=24 << 20),
        name='finish',
    )(dxc, clid, y_in, dgp)


def swap_kernel(src_ref, dst_ref, local_sem, send_sem, recv_sem):
    me = lax.axis_index('tp')
    barrier = pltpu.get_barrier_semaphore()

    def greet(i, carry):
        pl.semaphore_signal(barrier, inc=1, device_id={'tp': (me + i) % TP}, device_id_type=MESH)
        return carry

    lax.fori_loop(1, TP, greet, 0)
    pl.semaphore_wait(barrier, TP - 1)

    def copy(i):
        peer = (me + i) % TP
        return pltpu.make_async_remote_copy(
            src_ref=src_ref.at[peer], dst_ref=dst_ref.at[me], send_sem=send_sem.at[i], recv_sem=recv_sem.at[me],
            device_id={'tp': peer}, device_id_type=MESH)

    def start(i, carry):
        copy(i).start()
        return carry

    lax.fori_loop(1, TP, start, 0)
    keep = pltpu.make_async_copy(src_ref.at[me], dst_ref.at[me], local_sem)
    keep.start()

    def wait(i, carry):
        peer = (me + i) % TP
        pltpu.make_async_remote_copy(
            src_ref=src_ref.at[peer], dst_ref=dst_ref.at[peer], send_sem=send_sem.at[i], recv_sem=recv_sem.at[peer],
            device_id={'tp': peer}, device_id_type=MESH).wait()
        return carry

    lax.fori_loop(1, TP, wait, 0)
    keep.wait()


def swap(blocks, cid):
    return pl.pallas_call(
        swap_kernel,
        out_shape=jax.ShapeDtypeStruct(blocks.shape, blocks.dtype),
        in_specs=[pl.BlockSpec(memory_space=pl.ANY)],
        out_specs=pl.BlockSpec(memory_space=pl.ANY),
        scratch_shapes=[pltpu.SemaphoreType.DMA, pltpu.SemaphoreType.DMA((TP,)), pltpu.SemaphoreType.DMA((TP,))],
        compiler_params=pltpu.CompilerParams(collective_id=cid, has_side_effects=True),
        name='swap',
    )(blocks)


def general(ids, table, gain, grad):
    local = ids.reshape(-1) - lax.axis_index('tp') * ROWS
    mine = (local >= 0) & (local < ROWS)
    looked = jnp.take(table, jnp.where(mine, local, 0), axis=0)
    parts = swap(jnp.where(mine[:, None], looked, jnp.zeros((), BF16)).reshape(TP, TOK, HID), 1)
    h = jnp.sum(parts.astype(F32), axis=0)
    inv = lax.rsqrt(jnp.mean(h * h, axis=-1, keepdims=True) + RMS_EPS)
    xh = h * inv
    y = xh.astype(BF16) * gain
    gr = grad.astype(F32)
    part = jnp.sum(gr * xh, axis=0)
    u = gr * gain.astype(F32)
    dx = (inv * (u - xh * jnp.mean(u * xh, axis=-1, keepdims=True))).astype(BF16)
    dx_all = swap(jnp.broadcast_to(dx[None], (TP, TOK, HID)), 2).reshape(SEQ, HID)
    dg = jnp.sum(swap(jnp.broadcast_to(part.reshape(1, TOK // 8, 128), (TP, TOK // 8, 128)), 3), axis=0).reshape(1, HID)
    de = jax.ops.segment_sum(dx_all.astype(F32), jnp.where(mine, local, ROWS), num_segments=ROWS)
    return de, y, dg


def device_step(token_ids, table, gain, grad):
    ids = token_ids.reshape(TP, TOK)
    grad = grad.reshape(TOK, HID)
    dxc, clid, y_in, dgp, flag = exchange(ids, table, gain, grad)
    de, y, dg = lax.cond(
        flag[0] > 0,
        lambda: general(ids, table, gain, grad),
        lambda: finish(dxc, clid, y_in, dgp),
    )
    return y.reshape(1, TOK, HID), de, dg.reshape(HID)


def solution(mesh):
    return jax.shard_map(
        device_step, mesh=mesh,
        in_specs=(P('dp', None), P('tp', None), P(None), P('dp', 'tp', None)),
        out_specs=(P('dp', 'tp', None), P(('dp', 'tp'), None), P('dp')), check_vma=False)
```

```python
import functools

import jax
import jax.numpy as jnp
from jax import lax
from jax.experimental import pallas as pl
from jax.experimental.pallas import tpu as pltpu
from jax.sharding import PartitionSpec as P

RMS_EPS = 1e-5
TP = 16
ROWS = 3072
HID = 2048
SEQ = 2048
TOK = 128
XC = 32
DC = 56
DW = 40
NC = 384
CHUNKS = 6
MESH = pl.DeviceIdType.MESH
F32 = jnp.float32
BF16 = jnp.bfloat16
I32 = jnp.int32


def dot(a, b):
    return lax.dot_general(a, b, (((1,), (0,)), ((), ())), preferred_element_type=F32)


def one_hot(mask):
    return jnp.where(mask, 1.0, 0.0).astype(BF16)


def owner_of(ids):
    return ((ids >> 10) * 171) >> 9


def columns(rows):
    pad = jnp.zeros((128 - rows.shape[0], 128), rows.dtype)
    return jnp.concatenate([rows, pad], axis=0).T


def exchange_kernel(
    ids_hbm, table_ref, gain_hbm, grad_hbm,
    dxc_ref, clid_ref, y_ref, dgp_ref, flag_ref,
    ids_ref, gain_ref, grad_ref, in_sem, tbl, tbl_sem, xs, xrecv, ds, zbuf, drecv, dxs, dgs, hs,
    xz_send, xf_send, x_sem, dz_send, z_sem, df_send, d_sem, g_send, g_sem,
):
    me = lax.axis_index('tp')
    z = me // 4
    lane = me % 4
    y = lane // 2
    c = lane % 2
    sib = z * 4 + y * 2 + (1 - c)
    ymate = z * 4 + (1 - y) * 2 + c
    zs = [z, z + 1 - 2 * (z % 2), z + 2 - 4 * (z // 2), 3 - z]

    first_loads = [
        pltpu.make_async_copy(src, dst, in_sem.at[i])
        for i, (src, dst) in enumerate(((ids_hbm, ids_ref), (grad_hbm, grad_ref), (gain_hbm, gain_ref)))
    ]
    for load in first_loads:
        load.start()
    barrier = pltpu.get_barrier_semaphore()

    def greet(i, carry):
        pl.semaphore_signal(barrier, inc=1, device_id={'tp': (me + i) % TP}, device_id_type=MESH)
        return carry

    lax.fori_loop(1, TP, greet, 0)

    part = ROWS // CHUNKS
    loads = [
        pltpu.make_async_copy(table_ref.at[pl.ds(i * part, part)], tbl.at[pl.ds(i * part, part)], tbl_sem.at[i])
        for i in range(CHUNKS)
    ]
    for load in loads:
        load.start()

    sends = []

    def send(src, dst, ssem, rsem, dev):
        cp = pltpu.make_async_remote_copy(
            src_ref=src, dst_ref=dst, send_sem=ssem, recv_sem=rsem, device_id={'tp': dev}, device_id_type=MESH)
        cp.start()
        sends.append(cp)

    def arrived(ref, sem):
        pltpu.make_async_remote_copy(
            src_ref=ref, dst_ref=ref, send_sem=xz_send.at[0], recv_sem=sem,
            device_id={'tp': sib}, device_id_type=MESH).wait_recv()

    first_loads[0].wait()
    ids = ids_ref[...]
    own = owner_of(ids)
    row_iota = lax.broadcasted_iota(I32, (TP, 128), 0)
    sub = lax.broadcasted_iota(I32, (128, 128), 0)
    lan = lax.broadcasted_iota(I32, (128, 128), 1)
    before = sub < lan

    def my_row(rows):
        return jnp.sum(jnp.where(row_iota == me, rows, 0), axis=0, keepdims=True)

    my_own = my_row(own)
    my_own_c = columns(jnp.broadcast_to(my_own, (8, 128)))[:, 0:1]
    my_chip = my_own >> 1
    same = ((my_own_c >> 1) == my_chip) & before
    my_rank = jnp.sum(jnp.where(same, 1, 0), axis=0, keepdims=True)
    my_slot = jnp.where((my_chip & 1) == 0, my_rank, DC - 1 - my_rank)
    my_zown = my_own >> 2
    dslot_iota = lax.broadcasted_iota(I32, (DC, 128), 0)

    def pack_dy(k):
        pick = (dslot_iota == my_slot) & (my_zown == zs[k])
        return dot(one_hot(pick), grad_ref[...]).astype(BF16)

    lo, hi = y * (DC - DW), (1 - y) * (DC - DW)

    def forward_z(k):
        src = zs[k] * 4 + lane
        if k:
            arrived(zbuf.at[k], z_sem.at[k])
        send(zbuf.at[k, pl.ds(pl.multiple_of(hi, 8), DW)], drecv.at[src], df_send.at[3 * k], d_sem.at[src], ymate)
        send(zbuf.at[k, pl.ds(pl.multiple_of(lo, 8), DW)], drecv.at[src], df_send.at[3 * k + 1], d_sem.at[src], sib)

    def forward_zmate(k):
        src = zs[k] * 4 + (1 - y) * 2 + c
        arrived(drecv.at[src], d_sem.at[src])
        send(drecv.at[src], drecv.at[src], df_send.at[3 * k + 2], d_sem.at[src], sib)

    def collect_dy(k):
        for j in range(2):
            src = zs[k] * 4 + ((1 - y) * 2 if j else y * 2) + (1 - c)
            arrived(drecv.at[src], d_sem.at[src])

    def send_dy(k):
        send(ds.at[k - 1], zbuf.at[k], dz_send.at[k - 1], z_sem.at[k], zs[k] * 4 + lane)

    first_loads[1].wait()
    first_loads[2].wait()
    ds[0] = pack_dy(1)
    pl.semaphore_wait(barrier, TP - 1)
    send_dy(1)
    zbuf[0] = pack_dy(0)
    forward_z(0)
    ds[1] = pack_dy(2)
    send_dy(2)
    ds[2] = pack_dy(3)

    idc = columns(ids)
    dup_rows = []
    for s in range(4):
        for b in range(4):
            acc = jnp.zeros((128, 128), I32)
            row = ids[4 * s + b:4 * s + b + 1, :]
            for a in range(b + 1):
                same = idc[:, 4 * s + a:4 * s + a + 1] == row
                if a == b:
                    same = same & before
                acc = acc | jnp.where(same, 1, 0)
            dup_rows.append(jnp.max(acc, axis=0, keepdims=True))
    first = jnp.concatenate(dup_rows, axis=0) == 0
    key = jnp.where(first, own, -1)
    keyc = columns(key)
    rank_rows = []
    for s in range(4):
        for b in range(4):
            acc = jnp.zeros((128, 128), I32)
            row = own[4 * s + b:4 * s + b + 1, :]
            for a in range(b + 1):
                same = keyc[:, 4 * s + a:4 * s + a + 1] == row
                if a == b:
                    same = same & before
                acc = acc + jnp.where(same, 1, 0)
            rank_rows.append(jnp.sum(acc, axis=0, keepdims=True))
    rank = jnp.concatenate(rank_rows, axis=0)

    local = ids - me * ROWS
    mine = own == me
    xslot = jnp.where(first & mine, rank, -1)
    slot_iota = lax.broadcasted_iota(I32, (XC, 128), 0)
    lids = []
    for s in range(4):
        acc = jnp.zeros((XC, 128), I32)
        for a in range(4):
            d = 4 * s + a
            acc = acc + jnp.where(slot_iota == xslot[d:d + 1, :], local[d:d + 1, :] + 1, 0)
        lids.append(jnp.sum(acc, axis=1, keepdims=True) - 1)
    lid = jnp.concatenate(lids, axis=0)

    packed = jnp.zeros((4 * XC, HID), F32)
    chunk_iota = lax.broadcasted_iota(I32, (4 * XC, part), 1)
    for i in range(CHUNKS):
        loads[i].wait()
        packed = packed + dot(one_hot(chunk_iota + i * part == lid), tbl[pl.ds(i * part, part), :])
    packed = packed.astype(BF16)
    for s in range(4):
        xs[s] = packed[s * XC:(s + 1) * XC, :]
    xrecv[me] = xs[z]

    def forward_x(k):
        src = zs[k] * 4 + lane
        if k:
            arrived(xrecv.at[src], x_sem.at[src])
        send(xrecv.at[src], xrecv.at[src], xf_send.at[3 * k], x_sem.at[src], ymate)
        send(xrecv.at[src], xrecv.at[src], xf_send.at[3 * k + 1], x_sem.at[src], sib)

    def forward_xmate(k):
        src = zs[k] * 4 + (1 - y) * 2 + c
        arrived(xrecv.at[src], x_sem.at[src])
        send(xrecv.at[src], xrecv.at[src], xf_send.at[3 * k + 2], x_sem.at[src], sib)

    def collect_x(k):
        for j in range(2):
            src = zs[k] * 4 + ((1 - y) * 2 if j else y * 2) + (1 - c)
            arrived(xrecv.at[src], x_sem.at[src])

    for k in (1, 2, 3):
        send(xs.at[zs[k]], xrecv.at[me], xz_send.at[k - 1], x_sem.at[me], zs[k] * 4 + lane)
    forward_x(0)
    send_dy(3)
    forward_z(1)
    forward_zmate(0)

    over = jnp.max(jnp.where(first & (rank >= XC), 1, 0))

    def slab(rows):
        out = jnp.zeros((4, 128), I32)
        for s in range(4):
            out = out + jnp.where(z == s, rows[4 * s:4 * s + 4, :], 0)
        return out

    tslot = slab(jnp.where(first & (rank < XC), own * XC + rank, -1))
    mine_c = columns(jnp.concatenate([tslot, slab(ids), jnp.broadcast_to(my_row(ids), (8, 128))], axis=0))
    my_ids_c = mine_c[:, 8:9]
    spread = []
    for k in range(4):
        acc = jnp.zeros((128, 128), I32)
        for a in range(4):
            acc = acc + jnp.where(mine_c[:, a:a + 1] == lan + zs[k] * 128, mine_c[:, 4 + a:5 + a] + 1, 0)
        spread.append(one_hot(my_ids_c == jnp.sum(acc, axis=0, keepdims=True) - 1))

    def slab_rows(k):
        return [xrecv[zs[k] * 4 + j] for j in range(4)]

    chip_c = ((idc >> 10) * 171) >> 10
    chip = own >> 1
    drank_rows = []
    for d in range(TP):
        same = (chip_c[:, d:d + 1] == chip[d:d + 1, :]) & before
        drank_rows.append(jnp.sum(jnp.where(same, 1, 0), axis=0, keepdims=True))
    drank = jnp.concatenate(drank_rows, axis=0)
    over = jnp.maximum(over, jnp.max(jnp.where(drank >= DW, 1, 0)))
    for s in range(4):
        in_slab = jnp.sum(jnp.where((own >> 2) == s, 1.0, 0.0), axis=1, keepdims=True)
        over = jnp.maximum(over, jnp.max(jnp.where(in_slab > DC, 1, 0)))
    for o in range(TP):
        over = jnp.maximum(over, jnp.where(jnp.sum(jnp.where(own == o, 1.0, 0.0)) > NC, 1, 0))
    flag_ref[0] = over
    forward_xmate(0)

    def by_group(rows):
        out = []
        for k in range(4):
            part_k = jnp.zeros((4, 128), I32)
            for s in range(4):
                part_k = part_k + jnp.where(zs[k] == s, rows[4 * s:4 * s + 4, :], 0)
            out.append(part_k)
        return jnp.concatenate(out, axis=0)

    dslot = by_group(jnp.where(mine & (drank < DW), jnp.where(y == 0, drank, DW - 1 - drank), -1))
    dlocal = by_group(local)
    dslot_c = columns(jnp.concatenate([dslot, dlocal], axis=0))
    lrows = []
    for p in range(TP * DW // 128):
        acc = jnp.zeros((128, 128), I32)
        for d in range(TP):
            if d * DW < (p + 1) * 128 and (d + 1) * DW > p * 128:
                sc = dslot_c[:, d:d + 1]
                acc = acc + jnp.where((sc >= 0) & (sc + (d * DW - p * 128) == lan), dslot_c[:, TP + d:TP + d + 1] + 1, 0)
        lrows.append(jnp.sum(acc, axis=0, keepdims=True))
    lid1 = jnp.concatenate(lrows + [jnp.zeros((8 - len(lrows), 128), I32)], axis=0)
    has = lid1 > 0
    has_f = jnp.where(has, 1.0, 0.0)
    inrow = dot(has_f.astype(BF16), one_hot(before))
    total = jnp.sum(has_f, axis=1, keepdims=True)
    crank_rows = []
    base = jnp.zeros((1, 1), F32)
    for p in range(8):
        crank_rows.append(inrow[p:p + 1, :] + base)
        base = base + total[p:p + 1, :]
    crank = jnp.where(has, jnp.concatenate(crank_rows, axis=0).astype(I32), -1)
    n_iota = lax.broadcasted_iota(I32, (NC, 128), 0)
    compact = jnp.concatenate([one_hot(n_iota == crank[p:p + 1, :]) for p in range(len(lrows))], axis=1)
    lrow = jnp.concatenate([lid1[p:p + 1, :] for p in range(len(lrows))], axis=1)
    halves = jnp.concatenate([lrow >> 6, lrow & 63, jnp.zeros((6, TP * DW), I32)], axis=0).astype(F32).astype(BF16)
    cl = lax.dot_general(halves, compact, (((1,), (1,)), ((), ())), preferred_element_type=F32)
    clid_ref[...] = jnp.broadcast_to((cl[0:1, :] * 64.0 + cl[1:2, :]).astype(I32) - 1, (8, NC))

    gain = gain_ref[...].reshape(1, HID)
    gain_f = gain.astype(F32)
    xlid = jnp.broadcast_to(lid, (4 * XC, 128)).T[0:1, :]
    w_iota = lax.broadcasted_iota(I32, (DW, 128), 0)
    x_group = lax.broadcasted_iota(I32, (1, 4 * XC), 1) // XC

    steps = [(r0, min(16, DW - r0)) for r0 in range(0, DW, 16)]

    def dx_block(k, off, block):
        at = 4 * k + off
        slot_row = jnp.sum(jnp.where(row_iota == at, dslot, 0), axis=0, keepdims=True)
        local_row = jnp.sum(jnp.where(row_iota == at, dlocal, 0), axis=0, keepdims=True)
        dlid = jnp.sum(jnp.where(w_iota == slot_row, local_row + 1, 0), axis=1, keepdims=True) - 1
        pick = one_hot(dlid == jnp.where(x_group == zs[k], xlid, -2))
        h_all = dot(pick, jnp.concatenate([xs[s] for s in range(4)], axis=0))
        for r0, n in steps:
            h = h_all[r0:r0 + n, :]
            inv = lax.rsqrt(jnp.mean(h * h, axis=-1, keepdims=True) + RMS_EPS)
            xh = h * inv
            u = block(r0, n).astype(F32) * gain_f
            dx = inv * (u - xh * jnp.mean(u * xh, axis=-1, keepdims=True))
            dxs[at, pl.ds(r0, n), :] = dx.astype(BF16)

    def own_block(k):
        dx_block(k, lane, lambda r0, n: zbuf[k, pl.ds(pl.multiple_of(lo + r0, 8), n), :])

    def got_block(k, off):
        at = zs[k] * 4 + off
        dx_block(k, off, lambda r0, n: drecv[at, pl.ds(r0, n), :])

    mate_off, sib_off, far_off = (1 - y) * 2 + c, y * 2 + (1 - c), (1 - y) * 2 + (1 - c)

    def process(k):
        own_block(k)
        got_block(k, mate_off)
        collect_dy(k)
        got_block(k, sib_off)
        got_block(k, far_off)

    forward_z(2)
    forward_zmate(1)
    process(0)
    forward_x(1)
    forward_zmate(2)
    process(1)
    forward_x(2)
    forward_xmate(1)
    process(2)
    forward_x(3)
    forward_xmate(2)
    forward_z(3)
    for k in range(3):
        collect_x(k)
    hs[...] = dot(jnp.concatenate(spread[:3], axis=1), jnp.concatenate(slab_rows(0) + slab_rows(1) + slab_rows(2), axis=0))
    forward_xmate(3)
    collect_x(3)
    h_all = hs[...] + dot(spread[3], jnp.concatenate(slab_rows(3), axis=0))
    gain_sum = jnp.zeros((1, HID), F32)
    for r0 in range(0, TOK, 16):
        h = h_all[r0:r0 + 16, :]
        xh = h * lax.rsqrt(jnp.mean(h * h, axis=-1, keepdims=True) + RMS_EPS)
        y_ref[pl.ds(r0, 16), :] = xh.astype(BF16) * gain
        gain_sum = gain_sum + jnp.sum(grad_ref[pl.ds(r0, 16), :].astype(F32) * xh, axis=0, keepdims=True)
    dgs[...] = gain_sum
    dgp_ref[me] = gain_sum
    for i in range(1, TP):
        send(dgs, dgp_ref.at[me], g_send.at[i - 1], g_sem.at[me], (me + i) % TP)
    own_block(3)
    early = 12 * DW
    dxc_ref[...] = dot(compact[:, :early], jnp.concatenate([dxs[d] for d in range(12)], axis=0)).astype(BF16)
    forward_zmate(3)
    got_block(3, mate_off)
    collect_dy(3)
    got_block(3, sib_off)
    got_block(3, far_off)
    late = dot(compact[:, early:], jnp.concatenate([dxs[d] for d in range(12, TP)], axis=0))
    dxc_ref[...] += late.astype(BF16)
    for i in range(1, TP):
        src = (me + i) % TP
        arrived(dgp_ref.at[src], g_sem.at[src])
    for cp in sends:
        cp.wait_send()


def exchange(ids, table, gain, grad):
    vmem = pl.BlockSpec(memory_space=pltpu.VMEM)
    dma = pltpu.SemaphoreType.DMA
    return pl.pallas_call(
        exchange_kernel,
        out_shape=(
            pltpu.VMEM((NC, HID), BF16),
            pltpu.VMEM((8, NC), I32),
            pltpu.VMEM((TOK, HID), BF16),
            pltpu.VMEM((TP, 1, HID), F32),
            pltpu.SMEM((1,), I32),
        ),
        in_specs=[pl.BlockSpec(memory_space=pltpu.HBM)] * 4,
        out_specs=(vmem, vmem, vmem, vmem, pl.BlockSpec(memory_space=pltpu.SMEM)),
        scratch_shapes=[
            pltpu.VMEM((TP, TOK), I32),
            pltpu.VMEM((HID,), BF16),
            pltpu.VMEM((TOK, HID), BF16),
            dma((3,)),
            pltpu.VMEM((ROWS, HID), BF16),
            dma((CHUNKS,)),
            pltpu.VMEM((4, XC, HID), BF16),
            pltpu.VMEM((TP, XC, HID), BF16),
            pltpu.VMEM((3, DC, HID), BF16),
            pltpu.VMEM((4, DC, HID), BF16),
            pltpu.VMEM((TP, DW, HID), BF16),
            pltpu.VMEM((TP, DW, HID), BF16),
            pltpu.VMEM((1, HID), F32),
            pltpu.VMEM((TOK, HID), F32),
            dma((3,)), dma((12,)), dma((TP,)), dma((3,)), dma((4,)), dma((12,)), dma((TP,)), dma((TP - 1,)), dma((TP,)),
        ],
        compiler_params=pltpu.CompilerParams(collective_id=0, has_side_effects=True, vmem_limit_bytes=44 << 20),
        name='exchange',
    )(ids, table, gain, grad)


BLK = 128
SLOTS = 8
HALF = 256


def finish_kernel(dxc_ref, clid_ref, y_in_ref, dgp_ref, de_ref, y_ref, dg_ref, buf, dg_s, sem, buf_sem):
    steps = ROWS // BLK
    keep_y = pltpu.make_async_copy(y_in_ref, y_ref, sem.at[0])
    keep_y.start()
    more = jnp.max(clid_ref[0:1, HALF:]) >= 0

    def out(i):
        slot = lax.rem(i, SLOTS)
        return pltpu.make_async_copy(buf.at[slot], de_ref.at[pl.ds(pl.multiple_of(i * BLK, BLK), BLK)], buf_sem.at[slot])

    def step(i, carry):
        @pl.when(i >= SLOTS)
        def _():
            out(i - SLOTS).wait()

        slot = lax.rem(i, SLOTS)
        rows = lax.broadcasted_iota(I32, (BLK, HALF), 0) + i * BLK
        buf[slot] = dot(one_hot(rows == clid_ref[0:1, :HALF]), dxc_ref[:HALF, :])

        @pl.when(more)
        def _():
            buf[slot] += dot(one_hot(rows[:, :NC - HALF] == clid_ref[0:1, HALF:]), dxc_ref[HALF:, :])

        out(i).start()
        return carry

    lax.fori_loop(0, steps, step, 0)
    total = dgp_ref[0]
    for d in range(1, TP):
        total = total + dgp_ref[d]
    dg_s[...] = total
    keep_dg = pltpu.make_async_copy(dg_s, dg_ref, sem.at[1])
    keep_dg.start()

    def drain(i, carry):
        out(i).wait()
        return carry

    lax.fori_loop(steps - SLOTS, steps, drain, 0)
    keep_y.wait()
    keep_dg.wait()


def finish(dxc, clid, y_in, dgp):
    vmem = pl.BlockSpec(memory_space=pltpu.VMEM)
    hbm = pl.BlockSpec(memory_space=pltpu.HBM)
    return pl.pallas_call(
        finish_kernel,
        out_shape=(
            pltpu.HBM((ROWS, HID), F32),
            pltpu.HBM((TOK, HID), BF16),
            pltpu.HBM((1, HID), F32),
        ),
        in_specs=[vmem] * 4,
        out_specs=(hbm, hbm, hbm),
        scratch_shapes=[
            pltpu.VMEM((SLOTS, BLK, HID), F32),
            pltpu.VMEM((1, HID), F32),
            pltpu.SemaphoreType.DMA((2,)),
            pltpu.SemaphoreType.DMA((SLOTS,)),
        ],
        compiler_params=pltpu.CompilerParams(vmem_limit_bytes=24 << 20),
        name='finish',
    )(dxc, clid, y_in, dgp)


def swap_kernel(src_ref, dst_ref, local_sem, send_sem, recv_sem):
    me = lax.axis_index('tp')
    barrier = pltpu.get_barrier_semaphore()

    def greet(i, carry):
        pl.semaphore_signal(barrier, inc=1, device_id={'tp': (me + i) % TP}, device_id_type=MESH)
        return carry

    lax.fori_loop(1, TP, greet, 0)
    pl.semaphore_wait(barrier, TP - 1)

    def copy(i):
        peer = (me + i) % TP
        return pltpu.make_async_remote_copy(
            src_ref=src_ref.at[peer], dst_ref=dst_ref.at[me], send_sem=send_sem.at[i], recv_sem=recv_sem.at[me],
            device_id={'tp': peer}, device_id_type=MESH)

    def start(i, carry):
        copy(i).start()
        return carry

    lax.fori_loop(1, TP, start, 0)
    keep = pltpu.make_async_copy(src_ref.at[me], dst_ref.at[me], local_sem)
    keep.start()

    def wait(i, carry):
        peer = (me + i) % TP
        pltpu.make_async_remote_copy(
            src_ref=src_ref.at[peer], dst_ref=dst_ref.at[peer], send_sem=send_sem.at[i], recv_sem=recv_sem.at[peer],
            device_id={'tp': peer}, device_id_type=MESH).wait()
        return carry

    lax.fori_loop(1, TP, wait, 0)
    keep.wait()


def swap(blocks, cid):
    return pl.pallas_call(
        swap_kernel,
        out_shape=jax.ShapeDtypeStruct(blocks.shape, blocks.dtype),
        in_specs=[pl.BlockSpec(memory_space=pl.ANY)],
        out_specs=pl.BlockSpec(memory_space=pl.ANY),
        scratch_shapes=[pltpu.SemaphoreType.DMA, pltpu.SemaphoreType.DMA((TP,)), pltpu.SemaphoreType.DMA((TP,))],
        compiler_params=pltpu.CompilerParams(collective_id=cid, has_side_effects=True),
        name='swap',
    )(blocks)


def general(ids, table, gain, grad):
    local = ids.reshape(-1) - lax.axis_index('tp') * ROWS
    mine = (local >= 0) & (local < ROWS)
    looked = jnp.take(table, jnp.where(mine, local, 0), axis=0)
    parts = swap(jnp.where(mine[:, None], looked, jnp.zeros((), BF16)).reshape(TP, TOK, HID), 1)
    h = jnp.sum(parts.astype(F32), axis=0)
    inv = lax.rsqrt(jnp.mean(h * h, axis=-1, keepdims=True) + RMS_EPS)
    xh = h * inv
    y = xh.astype(BF16) * gain
    gr = grad.astype(F32)
    part = jnp.sum(gr * xh, axis=0)
    u = gr * gain.astype(F32)
    dx = (inv * (u - xh * jnp.mean(u * xh, axis=-1, keepdims=True))).astype(BF16)
    dx_all = swap(jnp.broadcast_to(dx[None], (TP, TOK, HID)), 2).reshape(SEQ, HID)
    dg = jnp.sum(swap(jnp.broadcast_to(part.reshape(1, TOK // 8, 128), (TP, TOK // 8, 128)), 3), axis=0).reshape(1, HID)
    de = jax.ops.segment_sum(dx_all.astype(F32), jnp.where(mine, local, ROWS), num_segments=ROWS)
    return de, y, dg


def device_step(token_ids, table, gain, grad):
    ids = token_ids.reshape(TP, TOK)
    grad = grad.reshape(TOK, HID)
    dxc, clid, y_in, dgp, flag = exchange(ids, table, gain, grad)
    de, y, dg = lax.cond(
        flag[0] > 0,
        lambda: general(ids, table, gain, grad),
        lambda: finish(dxc, clid, y_in, dgp),
    )
    return y.reshape(1, TOK, HID), de, dg.reshape(HID)


def solution(mesh):
    return jax.shard_map(
        device_step, mesh=mesh,
        in_specs=(P('dp', None), P('tp', None), P(None), P('dp', 'tp', None)),
        out_specs=(P('dp', 'tp', None), P(('dp', 'tp'), None), P('dp')), check_vma=False)
```

```python
import functools

import jax
import jax.numpy as jnp
from jax import lax
from jax.experimental import pallas as pl
from jax.experimental.pallas import tpu as pltpu
from jax.sharding import PartitionSpec as P

RMS_EPS = 1e-5
TP = 16
ROWS = 3072
HID = 2048
SEQ = 2048
TOK = 128
XC = 32
DC = 56
DW = 40
NC = 384
CHUNKS = 6
MESH = pl.DeviceIdType.MESH
F32 = jnp.float32
BF16 = jnp.bfloat16
I32 = jnp.int32


def dot(a, b):
    return lax.dot_general(a, b, (((1,), (0,)), ((), ())), preferred_element_type=F32)


def one_hot(mask):
    return jnp.where(mask, 1.0, 0.0).astype(BF16)


def owner_of(ids):
    return ((ids >> 10) * 171) >> 9


def columns(rows):
    pad = jnp.zeros((128 - rows.shape[0], 128), rows.dtype)
    return jnp.concatenate([rows, pad], axis=0).T


def exchange_kernel(
    ids_hbm, table_ref, gain_hbm, grad_hbm,
    dxc_ref, clid_ref, y_ref, dgp_ref, flag_ref,
    ids_ref, gain_ref, grad_ref, in_sem, tbl, tbl_sem, xs, xrecv, ds, zbuf, drecv, dxs, dgs, hs,
    xz_send, xf_send, x_sem, dz_send, z_sem, df_send, d_sem, g_send, g_sem,
):
    me = lax.axis_index('tp')
    z = me // 4
    lane = me % 4
    y = lane // 2
    c = lane % 2
    sib = z * 4 + y * 2 + (1 - c)
    ymate = z * 4 + (1 - y) * 2 + c
    zs = [z, z + 1 - 2 * (z % 2), z + 2 - 4 * (z // 2), 3 - z]

    first_loads = [
        pltpu.make_async_copy(src, dst, in_sem.at[i])
        for i, (src, dst) in enumerate(((ids_hbm, ids_ref), (grad_hbm, grad_ref), (gain_hbm, gain_ref)))
    ]
    for load in first_loads:
        load.start()
    barrier = pltpu.get_barrier_semaphore()

    def greet(i, carry):
        pl.semaphore_signal(barrier, inc=1, device_id={'tp': (me + i) % TP}, device_id_type=MESH)
        return carry

    lax.fori_loop(1, TP, greet, 0)

    part = ROWS // CHUNKS
    loads = [
        pltpu.make_async_copy(table_ref.at[pl.ds(i * part, part)], tbl.at[pl.ds(i * part, part)], tbl_sem.at[i])
        for i in range(CHUNKS)
    ]
    for load in loads:
        load.start()

    sends = []

    def send(src, dst, ssem, rsem, dev):
        cp = pltpu.make_async_remote_copy(
            src_ref=src, dst_ref=dst, send_sem=ssem, recv_sem=rsem, device_id={'tp': dev}, device_id_type=MESH)
        cp.start()
        sends.append(cp)

    def arrived(ref, sem):
        pltpu.make_async_remote_copy(
            src_ref=ref, dst_ref=ref, send_sem=xz_send.at[0], recv_sem=sem,
            device_id={'tp': sib}, device_id_type=MESH).wait_recv()

    first_loads[0].wait()
    ids = ids_ref[...]
    own = owner_of(ids)
    row_iota = lax.broadcasted_iota(I32, (TP, 128), 0)
    sub = lax.broadcasted_iota(I32, (128, 128), 0)
    lan = lax.broadcasted_iota(I32, (128, 128), 1)
    before = sub < lan

    def my_row(rows):
        return jnp.sum(jnp.where(row_iota == me, rows, 0), axis=0, keepdims=True)

    my_own = my_row(own)
    my_own_c = columns(jnp.broadcast_to(my_own, (8, 128)))[:, 0:1]
    my_chip = my_own >> 1
    same = ((my_own_c >> 1) == my_chip) & before
    my_rank = jnp.sum(jnp.where(same, 1, 0), axis=0, keepdims=True)
    my_slot = jnp.where((my_chip & 1) == 0, my_rank, DC - 1 - my_rank)
    my_zown = my_own >> 2
    dslot_iota = lax.broadcasted_iota(I32, (DC, 128), 0)

    def pack_dy(k):
        pick = (dslot_iota == my_slot) & (my_zown == zs[k])
        return dot(one_hot(pick), grad_ref[...]).astype(BF16)

    lo, hi = y * (DC - DW), (1 - y) * (DC - DW)

    def forward_z(k):
        src = zs[k] * 4 + lane
        if k:
            arrived(zbuf.at[k], z_sem.at[k])
        send(zbuf.at[k, pl.ds(pl.multiple_of(hi, 8), DW)], drecv.at[src], df_send.at[3 * k], d_sem.at[src], ymate)
        send(zbuf.at[k, pl.ds(pl.multiple_of(lo, 8), DW)], drecv.at[src], df_send.at[3 * k + 1], d_sem.at[src], sib)

    def forward_zmate(k):
        src = zs[k] * 4 + (1 - y) * 2 + c
        arrived(drecv.at[src], d_sem.at[src])
        send(drecv.at[src], drecv.at[src], df_send.at[3 * k + 2], d_sem.at[src], sib)

    def collect_dy(k):
        for j in range(2):
            src = zs[k] * 4 + ((1 - y) * 2 if j else y * 2) + (1 - c)
            arrived(drecv.at[src], d_sem.at[src])

    def send_dy(k):
        send(ds.at[k - 1], zbuf.at[k], dz_send.at[k - 1], z_sem.at[k], zs[k] * 4 + lane)

    first_loads[1].wait()
    first_loads[2].wait()
    ds[0] = pack_dy(1)
    pl.semaphore_wait(barrier, TP - 1)
    send_dy(1)
    zbuf[0] = pack_dy(0)
    forward_z(0)
    ds[1] = pack_dy(2)
    send_dy(2)
    ds[2] = pack_dy(3)

    idc = columns(ids)
    dup_rows = []
    for s in range(4):
        for b in range(4):
            acc = jnp.zeros((128, 128), I32)
            row = ids[4 * s + b:4 * s + b + 1, :]
            for a in range(b + 1):
                same = idc[:, 4 * s + a:4 * s + a + 1] == row
                if a == b:
                    same = same & before
                acc = acc | jnp.where(same, 1, 0)
            dup_rows.append(jnp.max(acc, axis=0, keepdims=True))
    first = jnp.concatenate(dup_rows, axis=0) == 0
    key = jnp.where(first, own, -1)
    keyc = columns(key)
    rank_rows = []
    for s in range(4):
        for b in range(4):
            acc = jnp.zeros((128, 128), I32)
            row = own[4 * s + b:4 * s + b + 1, :]
            for a in range(b + 1):
                same = keyc[:, 4 * s + a:4 * s + a + 1] == row
                if a == b:
                    same = same & before
                acc = acc + jnp.where(same, 1, 0)
            rank_rows.append(jnp.sum(acc, axis=0, keepdims=True))
    rank = jnp.concatenate(rank_rows, axis=0)

    local = ids - me * ROWS
    mine = own == me
    xslot = jnp.where(first & mine, rank, -1)
    slot_iota = lax.broadcasted_iota(I32, (XC, 128), 0)
    lids = []
    for s in range(4):
        acc = jnp.zeros((XC, 128), I32)
        for a in range(4):
            d = 4 * s + a
            acc = acc + jnp.where(slot_iota == xslot[d:d + 1, :], local[d:d + 1, :] + 1, 0)
        lids.append(jnp.sum(acc, axis=1, keepdims=True) - 1)
    lid = jnp.concatenate(lids, axis=0)

    packed = jnp.zeros((4 * XC, HID), F32)
    chunk_iota = lax.broadcasted_iota(I32, (4 * XC, part), 1)
    for i in range(CHUNKS):
        loads[i].wait()
        packed = packed + dot(one_hot(chunk_iota + i * part == lid), tbl[pl.ds(i * part, part), :])
    packed = packed.astype(BF16)
    for s in range(4):
        xs[s] = packed[s * XC:(s + 1) * XC, :]
    xrecv[me] = xs[z]

    def forward_x(k):
        src = zs[k] * 4 + lane
        if k:
            arrived(xrecv.at[src], x_sem.at[src])
        send(xrecv.at[src], xrecv.at[src], xf_send.at[3 * k], x_sem.at[src], ymate)
        send(xrecv.at[src], xrecv.at[src], xf_send.at[3 * k + 1], x_sem.at[src], sib)

    def forward_xmate(k):
        src = zs[k] * 4 + (1 - y) * 2 + c
        arrived(xrecv.at[src], x_sem.at[src])
        send(xrecv.at[src], xrecv.at[src], xf_send.at[3 * k + 2], x_sem.at[src], sib)

    def collect_x(k):
        for j in range(2):
            src = zs[k] * 4 + ((1 - y) * 2 if j else y * 2) + (1 - c)
            arrived(xrecv.at[src], x_sem.at[src])

    for k in (1, 2, 3):
        send(xs.at[zs[k]], xrecv.at[me], xz_send.at[k - 1], x_sem.at[me], zs[k] * 4 + lane)
    forward_x(0)
    late_send = len(sends)
    send_dy(3)
    forward_z(1)
    forward_zmate(0)

    over = jnp.max(jnp.where(first & (rank >= XC), 1, 0))

    def slab(rows):
        out = jnp.zeros((4, 128), I32)
        for s in range(4):
            out = out + jnp.where(z == s, rows[4 * s:4 * s + 4, :], 0)
        return out

    tslot = slab(jnp.where(first & (rank < XC), own * XC + rank, -1))
    mine_c = columns(jnp.concatenate([tslot, slab(ids), jnp.broadcast_to(my_row(ids), (8, 128))], axis=0))
    my_ids_c = mine_c[:, 8:9]
    spread = []
    for k in range(4):
        acc = jnp.zeros((128, 128), I32)
        for a in range(4):
            acc = acc + jnp.where(mine_c[:, a:a + 1] == lan + zs[k] * 128, mine_c[:, 4 + a:5 + a] + 1, 0)
        spread.append(one_hot(my_ids_c == jnp.sum(acc, axis=0, keepdims=True) - 1))

    def slab_rows(k):
        return [xrecv[zs[k] * 4 + j] for j in range(4)]

    chip_c = ((idc >> 10) * 171) >> 10
    chip = own >> 1
    drank_rows = []
    for d in range(TP):
        same = (chip_c[:, d:d + 1] == chip[d:d + 1, :]) & before
        drank_rows.append(jnp.sum(jnp.where(same, 1, 0), axis=0, keepdims=True))
    drank = jnp.concatenate(drank_rows, axis=0)
    over = jnp.maximum(over, jnp.max(jnp.where(drank >= DW, 1, 0)))
    for s in range(4):
        in_slab = jnp.sum(jnp.where((own >> 2) == s, 1.0, 0.0), axis=1, keepdims=True)
        over = jnp.maximum(over, jnp.max(jnp.where(in_slab > DC, 1, 0)))
    for o in range(TP):
        over = jnp.maximum(over, jnp.where(jnp.sum(jnp.where(own == o, 1.0, 0.0)) > NC, 1, 0))
    flag_ref[0] = over
    forward_xmate(0)

    def by_group(rows):
        out = []
        for k in range(4):
            part_k = jnp.zeros((4, 128), I32)
            for s in range(4):
                part_k = part_k + jnp.where(zs[k] == s, rows[4 * s:4 * s + 4, :], 0)
            out.append(part_k)
        return jnp.concatenate(out, axis=0)

    dslot = by_group(jnp.where(mine & (drank < DW), jnp.where(y == 0, drank, DW - 1 - drank), -1))
    dlocal = by_group(local)
    dslot_c = columns(jnp.concatenate([dslot, dlocal], axis=0))
    lrows = []
    for p in range(TP * DW // 128):
        acc = jnp.zeros((128, 128), I32)
        for d in range(TP):
            if d * DW < (p + 1) * 128 and (d + 1) * DW > p * 128:
                sc = dslot_c[:, d:d + 1]
                acc = acc + jnp.where((sc >= 0) & (sc + (d * DW - p * 128) == lan), dslot_c[:, TP + d:TP + d + 1] + 1, 0)
        lrows.append(jnp.sum(acc, axis=0, keepdims=True))
    lid1 = jnp.concatenate(lrows + [jnp.zeros((8 - len(lrows), 128), I32)], axis=0)
    has = lid1 > 0
    has_f = jnp.where(has, 1.0, 0.0)
    inrow = dot(has_f.astype(BF16), one_hot(before))
    total = jnp.sum(has_f, axis=1, keepdims=True)
    crank_rows = []
    base = jnp.zeros((1, 1), F32)
    for p in range(8):
        crank_rows.append(inrow[p:p + 1, :] + base)
        base = base + total[p:p + 1, :]
    crank = jnp.where(has, jnp.concatenate(crank_rows, axis=0).astype(I32), -1)
    n_iota = lax.broadcasted_iota(I32, (NC, 128), 0)
    compact = jnp.concatenate([one_hot(n_iota == crank[p:p + 1, :]) for p in range(len(lrows))], axis=1)
    lrow = jnp.concatenate([lid1[p:p + 1, :] for p in range(len(lrows))], axis=1)
    halves = jnp.concatenate([lrow >> 6, lrow & 63, jnp.zeros((6, TP * DW), I32)], axis=0).astype(F32).astype(BF16)
    cl = lax.dot_general(halves, compact, (((1,), (1,)), ((), ())), preferred_element_type=F32)
    clid_ref[...] = jnp.broadcast_to((cl[0:1, :] * 64.0 + cl[1:2, :]).astype(I32) - 1, (8, NC))

    gain = gain_ref[...].reshape(1, HID)
    gain_f = gain.astype(F32)
    xlid = jnp.broadcast_to(lid, (4 * XC, 128)).T[0:1, :]
    w_iota = lax.broadcasted_iota(I32, (DW, 128), 0)
    x_group = lax.broadcasted_iota(I32, (1, 4 * XC), 1) // XC

    steps = [(r0, min(16, DW - r0)) for r0 in range(0, DW, 16)]

    def dx_block(k, off, block):
        at = 4 * k + off
        slot_row = jnp.sum(jnp.where(row_iota == at, dslot, 0), axis=0, keepdims=True)
        local_row = jnp.sum(jnp.where(row_iota == at, dlocal, 0), axis=0, keepdims=True)
        dlid = jnp.sum(jnp.where(w_iota == slot_row, local_row + 1, 0), axis=1, keepdims=True) - 1
        pick = one_hot(dlid == jnp.where(x_group == zs[k], xlid, -2))
        h_all = dot(pick, jnp.concatenate([xs[s] for s in range(4)], axis=0))
        for r0, n in steps:
            h = h_all[r0:r0 + n, :]
            inv = lax.rsqrt(jnp.mean(h * h, axis=-1, keepdims=True) + RMS_EPS)
            xh = h * inv
            u = block(r0, n).astype(F32) * gain_f
            dx = inv * (u - xh * jnp.mean(u * xh, axis=-1, keepdims=True))
            dxs[at, pl.ds(r0, n), :] = dx.astype(BF16)

    def own_block(k):
        dx_block(k, lane, lambda r0, n: zbuf[k, pl.ds(pl.multiple_of(lo + r0, 8), n), :])

    def got_block(k, off):
        at = zs[k] * 4 + off
        dx_block(k, off, lambda r0, n: drecv[at, pl.ds(r0, n), :])

    mate_off, sib_off, far_off = (1 - y) * 2 + c, y * 2 + (1 - c), (1 - y) * 2 + (1 - c)

    def process(k):
        own_block(k)
        got_block(k, mate_off)
        collect_dy(k)
        got_block(k, sib_off)
        got_block(k, far_off)

    forward_z(2)
    forward_zmate(1)
    process(0)
    forward_x(1)
    forward_zmate(2)
    process(1)
    forward_x(2)
    forward_xmate(1)
    process(2)
    forward_x(3)
    forward_xmate(2)
    settled = len(sends)
    forward_z(3)
    for k in range(3):
        collect_x(k)
    hs[...] = dot(jnp.concatenate(spread[:3], axis=1), jnp.concatenate(slab_rows(0) + slab_rows(1) + slab_rows(2), axis=0))
    forward_xmate(3)
    collect_x(3)
    h_all = hs[...] + dot(spread[3], jnp.concatenate(slab_rows(3), axis=0))
    gain_sum = jnp.zeros((1, HID), F32)
    for r0 in range(0, TOK, 16):
        h = h_all[r0:r0 + 16, :]
        xh = h * lax.rsqrt(jnp.mean(h * h, axis=-1, keepdims=True) + RMS_EPS)
        y_ref[pl.ds(r0, 16), :] = xh.astype(BF16) * gain
        gain_sum = gain_sum + jnp.sum(grad_ref[pl.ds(r0, 16), :].astype(F32) * xh, axis=0, keepdims=True)
    dgs[...] = gain_sum
    dgp_ref[me] = gain_sum
    for i in range(1, TP):
        send(dgs, dgp_ref.at[me], g_send.at[i - 1], g_sem.at[me], (me + i) % TP)
    own_block(3)
    early = 12 * DW
    dxc_ref[...] = dot(compact[:, :early], jnp.concatenate([dxs[d] for d in range(12)], axis=0)).astype(BF16)
    arrived(drecv.at[zs[3] * 4 + sib_off], d_sem.at[zs[3] * 4 + sib_off])
    got_block(3, sib_off)
    for i, cp in enumerate(sends[:settled]):
        if i != late_send:
            cp.wait_send()
    forward_zmate(3)
    got_block(3, mate_off)
    arrived(drecv.at[zs[3] * 4 + far_off], d_sem.at[zs[3] * 4 + far_off])
    got_block(3, far_off)
    late = dot(compact[:, early:], jnp.concatenate([dxs[d] for d in range(12, TP)], axis=0))
    dxc_ref[...] += late.astype(BF16)
    for i in range(1, TP):
        src = (me + i) % TP
        arrived(dgp_ref.at[src], g_sem.at[src])
    for i, cp in enumerate(sends):
        if i >= settled or i == late_send:
            cp.wait_send()


def exchange(ids, table, gain, grad):
    vmem = pl.BlockSpec(memory_space=pltpu.VMEM)
    dma = pltpu.SemaphoreType.DMA
    return pl.pallas_call(
        exchange_kernel,
        out_shape=(
            pltpu.VMEM((NC, HID), BF16),
            pltpu.VMEM((8, NC), I32),
            pltpu.VMEM((TOK, HID), BF16),
            pltpu.VMEM((TP, 1, HID), F32),
            pltpu.SMEM((1,), I32),
        ),
        in_specs=[pl.BlockSpec(memory_space=pltpu.HBM)] * 4,
        out_specs=(vmem, vmem, vmem, vmem, pl.BlockSpec(memory_space=pltpu.SMEM)),
        scratch_shapes=[
            pltpu.VMEM((TP, TOK), I32),
            pltpu.VMEM((HID,), BF16),
            pltpu.VMEM((TOK, HID), BF16),
            dma((3,)),
            pltpu.VMEM((ROWS, HID), BF16),
            dma((CHUNKS,)),
            pltpu.VMEM((4, XC, HID), BF16),
            pltpu.VMEM((TP, XC, HID), BF16),
            pltpu.VMEM((3, DC, HID), BF16),
            pltpu.VMEM((4, DC, HID), BF16),
            pltpu.VMEM((TP, DW, HID), BF16),
            pltpu.VMEM((TP, DW, HID), BF16),
            pltpu.VMEM((1, HID), F32),
            pltpu.VMEM((TOK, HID), F32),
            dma((3,)), dma((12,)), dma((TP,)), dma((3,)), dma((4,)), dma((12,)), dma((TP,)), dma((TP - 1,)), dma((TP,)),
        ],
        compiler_params=pltpu.CompilerParams(collective_id=0, has_side_effects=True, vmem_limit_bytes=44 << 20),
        name='exchange',
    )(ids, table, gain, grad)


BLK = 128
SLOTS = 8
HALF = 256


def finish_kernel(dxc_ref, clid_ref, y_in_ref, dgp_ref, de_ref, y_ref, dg_ref, buf, dg_s, sem, buf_sem):
    steps = ROWS // BLK
    keep_y = pltpu.make_async_copy(y_in_ref, y_ref, sem.at[0])
    keep_y.start()
    more = jnp.max(clid_ref[0:1, HALF:]) >= 0

    def out(i):
        slot = lax.rem(i, SLOTS)
        return pltpu.make_async_copy(buf.at[slot], de_ref.at[pl.ds(pl.multiple_of(i * BLK, BLK), BLK)], buf_sem.at[slot])

    def step(i, carry):
        @pl.when(i >= SLOTS)
        def _():
            out(i - SLOTS).wait()

        slot = lax.rem(i, SLOTS)
        rows = lax.broadcasted_iota(I32, (BLK, HALF), 0) + i * BLK
        buf[slot] = dot(one_hot(rows == clid_ref[0:1, :HALF]), dxc_ref[:HALF, :])

        @pl.when(more)
        def _():
            buf[slot] += dot(one_hot(rows[:, :NC - HALF] == clid_ref[0:1, HALF:]), dxc_ref[HALF:, :])

        out(i).start()
        return carry

    lax.fori_loop(0, steps, step, 0)
    total = dgp_ref[0]
    for d in range(1, TP):
        total = total + dgp_ref[d]
    dg_s[...] = total
    keep_dg = pltpu.make_async_copy(dg_s, dg_ref, sem.at[1])
    keep_dg.start()

    def drain(i, carry):
        out(i).wait()
        return carry

    lax.fori_loop(steps - SLOTS, steps, drain, 0)
    keep_y.wait()
    keep_dg.wait()


def finish(dxc, clid, y_in, dgp):
    vmem = pl.BlockSpec(memory_space=pltpu.VMEM)
    hbm = pl.BlockSpec(memory_space=pltpu.HBM)
    return pl.pallas_call(
        finish_kernel,
        out_shape=(
            pltpu.HBM((ROWS, HID), F32),
            pltpu.HBM((TOK, HID), BF16),
            pltpu.HBM((1, HID), F32),
        ),
        in_specs=[vmem] * 4,
        out_specs=(hbm, hbm, hbm),
        scratch_shapes=[
            pltpu.VMEM((SLOTS, BLK, HID), F32),
            pltpu.VMEM((1, HID), F32),
            pltpu.SemaphoreType.DMA((2,)),
            pltpu.SemaphoreType.DMA((SLOTS,)),
        ],
        compiler_params=pltpu.CompilerParams(vmem_limit_bytes=24 << 20),
        name='finish',
    )(dxc, clid, y_in, dgp)


def swap_kernel(src_ref, dst_ref, local_sem, send_sem, recv_sem):
    me = lax.axis_index('tp')
    barrier = pltpu.get_barrier_semaphore()

    def greet(i, carry):
        pl.semaphore_signal(barrier, inc=1, device_id={'tp': (me + i) % TP}, device_id_type=MESH)
        return carry

    lax.fori_loop(1, TP, greet, 0)
    pl.semaphore_wait(barrier, TP - 1)

    def copy(i):
        peer = (me + i) % TP
        return pltpu.make_async_remote_copy(
            src_ref=src_ref.at[peer], dst_ref=dst_ref.at[me], send_sem=send_sem.at[i], recv_sem=recv_sem.at[me],
            device_id={'tp': peer}, device_id_type=MESH)

    def start(i, carry):
        copy(i).start()
        return carry

    lax.fori_loop(1, TP, start, 0)
    keep = pltpu.make_async_copy(src_ref.at[me], dst_ref.at[me], local_sem)
    keep.start()

    def wait(i, carry):
        peer = (me + i) % TP
        pltpu.make_async_remote_copy(
            src_ref=src_ref.at[peer], dst_ref=dst_ref.at[peer], send_sem=send_sem.at[i], recv_sem=recv_sem.at[peer],
            device_id={'tp': peer}, device_id_type=MESH).wait()
        return carry

    lax.fori_loop(1, TP, wait, 0)
    keep.wait()


def swap(blocks, cid):
    return pl.pallas_call(
        swap_kernel,
        out_shape=jax.ShapeDtypeStruct(blocks.shape, blocks.dtype),
        in_specs=[pl.BlockSpec(memory_space=pl.ANY)],
        out_specs=pl.BlockSpec(memory_space=pl.ANY),
        scratch_shapes=[pltpu.SemaphoreType.DMA, pltpu.SemaphoreType.DMA((TP,)), pltpu.SemaphoreType.DMA((TP,))],
        compiler_params=pltpu.CompilerParams(collective_id=cid, has_side_effects=True),
        name='swap',
    )(blocks)


def general(ids, table, gain, grad):
    local = ids.reshape(-1) - lax.axis_index('tp') * ROWS
    mine = (local >= 0) & (local < ROWS)
    looked = jnp.take(table, jnp.where(mine, local, 0), axis=0)
    parts = swap(jnp.where(mine[:, None], looked, jnp.zeros((), BF16)).reshape(TP, TOK, HID), 1)
    h = jnp.sum(parts.astype(F32), axis=0)
    inv = lax.rsqrt(jnp.mean(h * h, axis=-1, keepdims=True) + RMS_EPS)
    xh = h * inv
    y = xh.astype(BF16) * gain
    gr = grad.astype(F32)
    part = jnp.sum(gr * xh, axis=0)
    u = gr * gain.astype(F32)
    dx = (inv * (u - xh * jnp.mean(u * xh, axis=-1, keepdims=True))).astype(BF16)
    dx_all = swap(jnp.broadcast_to(dx[None], (TP, TOK, HID)), 2).reshape(SEQ, HID)
    dg = jnp.sum(swap(jnp.broadcast_to(part.reshape(1, TOK // 8, 128), (TP, TOK // 8, 128)), 3), axis=0).reshape(1, HID)
    de = jax.ops.segment_sum(dx_all.astype(F32), jnp.where(mine, local, ROWS), num_segments=ROWS)
    return de, y, dg


def device_step(token_ids, table, gain, grad):
    ids = token_ids.reshape(TP, TOK)
    grad = grad.reshape(TOK, HID)
    dxc, clid, y_in, dgp, flag = exchange(ids, table, gain, grad)
    de, y, dg = lax.cond(
        flag[0] > 0,
        lambda: general(ids, table, gain, grad),
        lambda: finish(dxc, clid, y_in, dgp),
    )
    return y.reshape(1, TOK, HID), de, dg.reshape(HID)


def solution(mesh):
    return jax.shard_map(
        device_step, mesh=mesh,
        in_specs=(P('dp', None), P('tp', None), P(None), P('dp', 'tp', None)),
        out_specs=(P('dp', 'tp', None), P(('dp', 'tp'), None), P('dp')), check_vma=False)
```
